32 devices in a mesh: ty: 4 (over z), tx: 8 (over y, x, core).
Axes of the slice: x: 2, y: 2, z: 4, core: 2. Of those that a mesh axis runs over, the one named last changes fastest.
Arguments:
- object_slices: float32 [2, 2, 2048, 4096], P(None, None, 'ty', 'tx'), may hold values from -4 to 4
- probe_modes: float32 [4, 2, 128, 128], replicated, may hold values from -12 to 12
- patterns: bfloat16 [256, 128, 128], P(('ty', 'tx')), may hold values from 0 to 2
- positions: int32 [256, 2], replicated, may hold values from 0 to 4095, as said below
- counts: int32 [32], replicated, may hold values from 6 to 8, as said below
Outputs:
- new_object: float32 [2, 2, 2048, 4096], P(None, None, 'ty', 'tx')
- new_probe: float32 [4, 2, 128, 128], replicated
The draws below stay inside these ranges and needn't reach their ends.
Inputs may be any that keep to these rules, and one draw needn't show every extreme that they name: positions[j] is the centre of pattern j, which was acquired by device j // 8 of ty+tx (ty slowest); its column lies in that device's column of tiles of 512 x 512 cells. Of the live patterns of one device, at most 2 lie in any one row of tiles; in every column of tiles some row of tiles holds exactly 2 live patterns from every device of that column. The live patterns of device d are its first counts[d] slots; some device has 8.
All inputs are finite; a program needn't handle non-finite values.
Results may differ from the reference program's by a relative error of at most 0.0085.
The reference program's roundings to bfloat16 on the way count: a program that leaves them out, or rounds other values in their place, can miss the bound.
Values may be sent and summed in bfloat16 or wider, within the bound.
No kernel may reach another device: no remote copies, remote signals or barrier semaphores. Data moves between devices by JAX's collectives and lax.ppermute only.
A program may use at most 128 MiB of HBM per device.

```python
import math
import jax
import jax.numpy as jnp
from jax import lax

P_SIZE = 128
MODES = 4
SLICES = 2
TILE = 512
PAT_DEV = 8
CAP = 2
NY = 2048
NX = 4096
PATTERNS = 256
N_TY = 4
N_TX = 8


def routing_plan(key):
    devices = N_TY * N_TX
    key_list = jax.random.split(jax.random.fold_in(key, 4242), 7)
    counts = jax.random.randint(key_list[0], (devices,), PAT_DEV - 2, PAT_DEV + 1)
    chosen = jax.random.randint(key_list[1], (), 0, devices)
    counts = jnp.where(jnp.arange(devices) == chosen, PAT_DEV, counts).astype(jnp.int32)
    hot_rows = jax.random.randint(key_list[2], (N_TX,), 0, N_TY)
    columns = jnp.arange(devices) % N_TX
    device_hot = hot_rows[columns]
    spare = (N_TY - 1) * CAP
    offsets = jnp.arange(spare) // CAP
    others = (device_hot[:, None] + 1 + offsets[None, :]) % N_TY
    scores = jax.random.randint(key_list[3], (devices, spare), 0, 2 ** 20) * spare + jnp.arange(spare)[None, :]
    permuted = jnp.argsort(scores, axis=1)
    picked = jnp.take_along_axis(others, permuted, axis=1)[:, :PAT_DEV - CAP]
    listed = jnp.concatenate([jnp.broadcast_to(device_hot[:, None], (devices, CAP)), picked], axis=1)
    slot_ids = jnp.arange(PAT_DEV)
    order_scores = jax.random.randint(key_list[4], (devices, PAT_DEV), 0, 2 ** 20) * PAT_DEV + slot_ids[None, :]
    order_scores = jnp.where(slot_ids[None, :] >= counts[:, None], 2 ** 30 + slot_ids[None, :], order_scores)
    arrangement = jnp.argsort(order_scores, axis=1)
    dest_rows = jnp.take_along_axis(listed, arrangement, axis=1)
    rows_inside = jax.random.randint(key_list[5], (devices, PAT_DEV), 0, TILE)
    cols_inside = jax.random.randint(key_list[6], (devices, PAT_DEV), 0, TILE)
    centre_rows = dest_rows * TILE + rows_inside
    centre_cols = columns[:, None] * TILE + cols_inside
    positions = jnp.stack([centre_rows, centre_cols], -1).reshape(devices * PAT_DEV, 2).astype(jnp.int32)
    return (positions, counts)


def draw_positions(key, part):
    return routing_plan(key)[0]


def draw_counts(key, part):
    return routing_plan(key)[1]


def draw_probe_modes(key, part):
    normal_key = jax.random.fold_in(jax.random.fold_in(key, 77), 0)
    values = jnp.clip(jax.random.normal(normal_key, (MODES, 2, P_SIZE, P_SIZE), jnp.float32), -4.0, 4.0)
    decay = 0.6 * jnp.exp(-0.6 * jnp.arange(MODES, dtype=jnp.float32))
    values = values * decay[:, None, None, None]
    return values.astype(jnp.float32)


def block_levels(own_key, shape, pieces, low, top_value):
    factor_of = 1.0
    for axis_at, parts in pieces:
        heights = jax.random.uniform(jax.random.fold_in(jax.random.fold_in(own_key, 6), axis_at), (parts,), jnp.float32, low / len(pieces), top_value / len(pieces))
        factor_of = factor_of * jnp.repeat(jnp.exp(heights), shape[axis_at] // parts).reshape((-1,) + (1,) * (len(shape) - 1 - axis_at))
    return factor_of


def noise(key, shape, scale, most, shards=(), kind=jnp.bfloat16):
    drawn = jax.random.normal(key, shape, jnp.float32) * scale
    if len(shards) > 0:
        drawn = block_levels(key, shape, shards, -0.22, 0.18) * drawn
    return jnp.clip(drawn, min=-most, max=most).astype(kind)


def setup_inputs(seed: int = 0) -> dict:
    arg_keys = jax.random.split(jax.random.key(seed), 6)
    object_slices = noise(arg_keys[0], (SLICES, 2, NY, NX), 0.7, 4.0, ((2, 4), (3, 8)), jnp.float32)
    probe_modes = draw_probe_modes(jax.random.fold_in(arg_keys[5], 71), 0)
    patterns = jnp.clip(2.0 * jax.random.uniform(arg_keys[2], (PATTERNS, P_SIZE, P_SIZE), jnp.float32) ** block_levels(arg_keys[2], (PATTERNS, P_SIZE, P_SIZE), ((0, 32),), -0.2, 0.2), 0.0, 2.0).astype(jnp.bfloat16)
    positions = draw_positions(jax.random.fold_in(arg_keys[5], 71), 0)
    counts = draw_counts(jax.random.fold_in(arg_keys[5], 71), 0)
    return {"object_slices": object_slices, "probe_modes": probe_modes, "patterns": patterns, "positions": positions, "counts": counts}


PROPAGATION = 0.37

def make_tables(extent):
    indices = jnp.arange(extent, dtype=jnp.int32)
    product = indices[:, None] * indices[None, :] % extent
    angles = 2.0 * jnp.pi / extent * product.astype(jnp.float32)
    norm_scale = 1.0 / math.sqrt(extent)
    real_table = (jnp.cos(angles) * norm_scale).astype(jnp.bfloat16)
    imag_table = (-jnp.sin(angles) * norm_scale).astype(jnp.bfloat16)
    right_fwd = jnp.concatenate([jnp.concatenate([real_table, imag_table], 1), jnp.concatenate([-imag_table, real_table], 1)], 0)
    right_inv = jnp.concatenate([jnp.concatenate([real_table, -imag_table], 1), jnp.concatenate([imag_table, real_table], 1)], 0)
    left_fwd = jnp.concatenate([real_table, imag_table], 0)
    left_inv = jnp.concatenate([real_table, -imag_table], 0)
    frequency = jnp.where(indices < extent // 2, indices, indices - extent).astype(jnp.float32)
    phases = -jnp.pi * PROPAGATION / extent * (frequency[:, None] ** 2 + frequency[None, :] ** 2)
    kernel = jnp.stack([jnp.cos(phases), jnp.sin(phases)])
    return (right_fwd, left_fwd, right_inv, left_inv, kernel)

def transform(wave_field, right_table, left_table):
    extent = wave_field.shape[-1]
    rounded = wave_field.astype(jnp.bfloat16)
    joined = jnp.concatenate([rounded[:, 0], rounded[:, 1]], axis=-1)
    partial_value = jnp.einsum('bpk,kq->bpq', joined.astype(jnp.float32), right_table.astype(jnp.float32))
    partial_value = partial_value.astype(jnp.bfloat16)
    stacked = jnp.einsum('ij,bjq->biq', left_table.astype(jnp.float32), partial_value.astype(jnp.float32))
    real_part = stacked[:, :extent, :extent] - stacked[:, extent:, extent:]
    imag_part = stacked[:, extent:, :extent] + stacked[:, :extent, extent:]
    return jnp.stack([real_part, imag_part], axis=1)

def complex_product(former, latter):
    former_re = former[..., 0, :, :]
    former_im = former[..., 1, :, :]
    latter_re = latter[..., 0, :, :]
    latter_im = latter[..., 1, :, :]
    return jnp.stack([former_re * latter_re - former_im * latter_im, former_re * latter_im + former_im * latter_re], axis=-3)

def conjugate(values):
    return jnp.stack([values[..., 0, :, :], -values[..., 1, :, :]], axis=-3)

def pattern_terms(window, amplitude, live_flag, probe_modes, tables):
    right_fwd, left_fwd, right_inv, left_inv, kernel = tables
    slices = window.shape[0]
    inputs = [probe_modes]
    far_field = None
    for slice_index in range(slices):
        exit_wave = complex_product(inputs[slice_index], window[slice_index])
        if slice_index + 1 < slices:
            spread_wave = complex_product(kernel, transform(exit_wave, right_fwd, left_fwd))
            inputs.append(transform(spread_wave, right_inv, left_inv))
        else:
            far_field = transform(exit_wave, right_fwd, left_fwd)
    intensity = lax.optimization_barrier(jnp.sum(far_field[:, 0] ** 2 + far_field[:, 1] ** 2, axis=0))
    factor = (1.0 - amplitude / jnp.sqrt(jnp.maximum(intensity, 0.25))) * live_flag
    residue = far_field * factor
    backward = transform(residue, right_inv, left_inv)
    slice_grads = [None] * slices
    for slice_index in reversed(range(slices)):
        slice_grads[slice_index] = lax.optimization_barrier(jnp.sum(complex_product(conjugate(inputs[slice_index]), backward), axis=0))
        if slice_index > 0:
            inner_wave = transform(complex_product(conjugate(window[slice_index]), backward), right_fwd, left_fwd)
            backward = transform(complex_product(conjugate(kernel), inner_wave), right_inv, left_inv)
    probe_term = complex_product(conjugate(window[0]), backward)
    return (jnp.stack(slice_grads), probe_term)

def reference(object_slices, probe_modes, patterns, positions, counts):
    margin = P_SIZE // 2
    tables = make_tables(P_SIZE)
    padded = jnp.pad(object_slices, ((0, 0), (0, 0), (margin, margin), (margin, margin)))
    total_count = PAT_DEV * N_TY * N_TX
    ordinal = jnp.arange(total_count, dtype=jnp.int32)
    is_live = ordinal % PAT_DEV < jnp.repeat(counts, PAT_DEV)

    def visit_slot(running, element):
        gradient, probe_grad = running
        amplitude, place, live_now = element
        corner = (jnp.int32(0), jnp.int32(0), place[0].astype(jnp.int32), place[1].astype(jnp.int32))

        def compute_terms(operand):
            window = lax.dynamic_slice(padded, corner, (SLICES, 2, P_SIZE, P_SIZE))
            return pattern_terms(window, amplitude.astype(jnp.float32), 1.0, probe_modes, tables)

        def skip_terms(operand):
            return (jnp.zeros((SLICES, 2, P_SIZE, P_SIZE), jnp.float32), jnp.zeros((MODES, 2, P_SIZE, P_SIZE), jnp.float32))
        slice_grads, probe_term = lax.cond(live_now, compute_terms, skip_terms, 0)
        current = lax.dynamic_slice(gradient, corner, (SLICES, 2, P_SIZE, P_SIZE))
        gradient = lax.dynamic_update_slice(gradient, current + slice_grads, corner)
        return ((gradient, probe_grad + probe_term), None)
    initial = (jnp.zeros(padded.shape, jnp.float32), jnp.zeros((MODES, 2, P_SIZE, P_SIZE), jnp.float32))
    (gradient, probe_grad), unused = lax.scan(visit_slot, initial, (patterns, positions, is_live))
    gradient = gradient[:, :, margin:margin + NY, margin:margin + NX]
    probe_power = jnp.mean(lax.optimization_barrier(jnp.sum(probe_modes ** 2, axis=(0, 1))))
    new_object = object_slices - gradient / (probe_power + 1e-06)
    spread = jnp.sqrt(jnp.mean(probe_grad ** 2) + 1e-06)
    new_probe = probe_modes - 0.5 * probe_grad / spread
    return (new_object, new_probe)
```

```python
import math

import numpy as np
import jax
import jax.numpy as jnp
from jax import lax
from jax.experimental import pallas as pl
from jax.experimental.pallas import tpu as pltpu
from jax.sharding import PartitionSpec as P

CAP = 2
PROPAGATION = 0.37
LANES = 128
BF16 = jnp.bfloat16
F32 = jnp.float32


def make_tables(extent):
    indices = np.arange(extent, dtype=np.int32)
    product = indices[:, None] * indices[None, :] % extent
    angles = np.float32(2.0 * math.pi / extent) * product.astype(np.float32)
    norm_scale = np.float32(1.0 / math.sqrt(extent))
    real_table = jnp.asarray(np.cos(angles) * norm_scale, F32).astype(BF16)
    imag_table = jnp.asarray(-np.sin(angles) * norm_scale, F32).astype(BF16)
    first = jnp.concatenate(
        [
            jnp.concatenate([real_table, imag_table], 1),
            jnp.concatenate([-imag_table, real_table], 1),
        ],
        0,
    )
    second = jnp.concatenate(
        [
            jnp.concatenate([real_table, -imag_table], 1),
            jnp.concatenate([imag_table, real_table], 1),
        ],
        0,
    )
    frequency = np.where(indices < extent // 2, indices, indices - extent).astype(np.float32)
    phases = np.float32(-math.pi * PROPAGATION / extent) * (
        frequency[:, None] ** 2 + frequency[None, :] ** 2
    )
    kernel = jnp.asarray(np.stack([np.cos(phases), np.sin(phases)]), F32)
    return first, second, kernel


def pairings(n):
    if n == 2:
        return [[1, 0]]
    assert n % 2 == 0 and all((n - 1) % d for d in range(2, n - 1))
    odd = n - 1
    rounds = []
    for k in range(odd):
        partner = [0] * n
        partner[odd], partner[k] = k, odd
        for i in range(1, n // 2):
            a, b = (k + i) % odd, (k - i) % odd
            partner[a], partner[b] = b, a
        rounds.append(partner)
    order = [odd]
    while len(order) < n:
        order.append(rounds[(len(order) - 1) % 2][order[-1]])
    label = {v: i for i, v in enumerate(order)}
    return [[label[r[order[i]]] for i in range(n)] for r in rounds]


def neighbour(side, i):
    return 1 if (i + side) % 2 == 0 else -1


def neighbour_pairs(side, n):
    steps = [(i, i + neighbour(side, i)) for i in range(n)]
    return [(i, j) for i, j in steps if 0 <= j < n]


def pick(index, values):
    chosen = jnp.int32(values[0])
    for i in range(1, len(values)):
        chosen = jnp.where(index == i, jnp.int32(values[i]), chosen)
    return chosen


def lane_ids(rows):
    return lax.broadcasted_iota(jnp.int32, (rows, LANES), 1)


def half_mask(rows, upper):
    return (lane_ids(rows) >= LANES // 2).astype(jnp.int32) == upper


def ups(index):
    even = 1 - lax.rem(index, 2)
    return [even, 1 - even]


def pack_kernel(sizes, obj, pat, pos, cnt, *outs):
    n_ty, n_tx, rounds = sizes
    ty_out, tx_out, diag_out = outs[: len(rounds)], outs[len(rounds) : len(rounds) + 2], outs[len(rounds) + 2 :]
    slices, tile, extent = obj.shape[0], obj.shape[2], pat.shape[1]
    margin, tiles = extent // 2, obj.shape[3] // LANES
    row, col = lax.axis_index("ty"), lax.axis_index("tx")
    up_y, up_x = ups(row), ups(col)
    base = (row * n_tx + col) * pat.shape[0]
    count = cnt[row * n_tx + col]
    parts = slices * 2 * tiles
    for k, partner in enumerate(rounds):
        out = ty_out[k]
        if k < 2:
            start = pl.multiple_of(up_y[k] * (tile - margin), margin)
            nxt = row + 2 * up_y[k] - 1
            keep = jnp.where((nxt >= 0) & (nxt < n_ty), 1.0, 0.0).astype(F32)
            for p in range(slices * 2):
                for t in range(tiles):
                    block = obj[p // 2, p % 2, pl.ds(start, margin), t * LANES : (t + 1) * LANES]
                    out[p * tiles + t] = (block * keep).astype(BF16)
        low = pick(row, partner) * tile
        found = [jnp.int32(0)] * CAP
        seen = jnp.int32(0)
        for i in range(pat.shape[0]):
            y = pos[base + i, 0]
            hit = (i < count) & (y >= low) & (y < low + tile)
            for c in range(CAP):
                found[c] = jnp.where(hit & (seen == c), i, found[c])
            seen = seen + hit.astype(jnp.int32)
        first = parts if k < 2 else 0
        for c in range(CAP):
            for h in range(2):
                out[first + 2 * c + h] = pat[found[c], h * margin : (h + 1) * margin, :]
    for j in range(2):
        lane = pl.multiple_of(up_x[j] * (tile - LANES), LANES)
        for s in range(slices):
            re = obj[s, 0, :, pl.ds(lane, LANES)]
            im = obj[s, 1, :, pl.ds(lane, LANES)]
            packed = jnp.where(half_mask(tile, up_x[j]), re, pltpu.roll(im, LANES // 2, 1))
            tx_out[j][s] = packed.astype(BF16)
            for k in range(2):
                start = pl.multiple_of(up_y[k] * (tile - margin), margin)
                re = obj[s, 0, pl.ds(start, margin), pl.ds(lane, LANES)]
                im = obj[s, 1, pl.ds(start, margin), pl.ds(lane, LANES)]
                packed = jnp.where(half_mask(margin, up_x[j]), re, pltpu.roll(im, LANES // 2, 1))
                diag_out[2 * k + j][s] = packed.astype(BF16)


def cmul(a, b):
    return a[0] * b[0] - a[1] * b[1], a[0] * b[1] + a[1] * b[0]


def cmul_conj(a, b):
    return a[0] * b[0] + a[1] * b[1], a[0] * b[1] - a[1] * b[0]


def transform(fields, right, left):
    extent = fields[0][0].shape[0]
    joined = jnp.concatenate([jnp.concatenate([re, im], 1) for re, im in fields], 0).astype(BF16)
    half = jnp.dot(joined, right, preferred_element_type=F32).astype(BF16)
    blocks = []
    for m in range(len(fields)):
        part = half[m * extent : (m + 1) * extent]
        blocks.append(jnp.concatenate([part[:, :extent], part[:, extent:]], 0))
    whole = jnp.dot(left, jnp.concatenate(blocks, 1), preferred_element_type=F32)
    return [
        (whole[:extent, m * extent : (m + 1) * extent], whole[extent:, m * extent : (m + 1) * extent])
        for m in range(len(fields))
    ]


def main_kernel(sizes, obj, pat, pos, cnt, probe, first, second, kern, *refs):
    n_ty, n_tx, rounds = sizes
    k_n = len(rounds)
    ty_in, tx_in, diag_in = refs[:k_n], refs[k_n : k_n + 2], refs[k_n + 2 : k_n + 6]
    refs = refs[k_n + 6 :]
    grad, probe_grad, ty_out, tx_out, diag_out = refs[0], refs[1], refs[2:4], refs[4:6], refs[6:10]
    ext, amp, acc, row_of, col_of, live_of = refs[10:]
    slices, tile, extent = obj.shape[0], obj.shape[2], pat.shape[1]
    modes = probe.shape[0]
    margin, tiles = extent // 2, obj.shape[3] // LANES
    parts = slices * 2 * tiles
    per_device = pat.shape[0]
    row, col = lax.axis_index("ty"), lax.axis_index("tx")
    up_y, up_x = ups(row), ups(col)

    low, left = row * tile, col * tile
    for k in range(k_n + 1):
        source = row if k == 0 else pick(row, rounds[k - 1])
        base = (source * n_tx + col) * per_device
        count = cnt[source * n_tx + col]
        ys, xs = [jnp.int32(0)] * CAP, [jnp.int32(0)] * CAP
        lives, found = [jnp.float32(0)] * CAP, [jnp.int32(0)] * CAP
        seen = jnp.int32(0)
        for i in range(per_device):
            y, x = pos[base + i, 0], pos[base + i, 1]
            hit = (i < count) & (y >= low) & (y < low + tile)
            for c in range(CAP):
                this = hit & (seen == c)
                ys[c] = jnp.where(this, y - low, ys[c])
                xs[c] = jnp.where(this, x - left, xs[c])
                lives[c] = jnp.where(this, 1.0, lives[c])
                found[c] = jnp.where(this, i, found[c])
            seen = seen + hit.astype(jnp.int32)
        for c in range(CAP):
            slot = k * CAP + c
            row_of[slot], col_of[slot], live_of[slot] = ys[c], xs[c], lives[c]
            if k == 0:
                amp[slot] = pat[found[c]]
            else:
                start = (parts if k < 3 else 0) + 2 * c
                for h in range(2):
                    amp[slot, h * margin : (h + 1) * margin] = ty_in[k - 1][start + h]

    for p in range(slices * 2):
        for t in range(tiles):
            ext[p, 1 + t, margin : margin + tile] = obj[p // 2, p % 2, :, t * LANES : (t + 1) * LANES]
            for k in range(2):
                start = pl.multiple_of(up_y[k] * (tile + margin), margin)
                ext[p, 1 + t, pl.ds(start, margin)] = ty_in[k][p * tiles + t].astype(F32)
    for s in range(slices):
        for j in range(2):
            side = up_x[j] * (tiles + 1)
            strip = tx_in[j][s].astype(F32)
            ext[2 * s, side, margin : margin + tile] = strip
            ext[2 * s + 1, side, margin : margin + tile] = pltpu.roll(strip, LANES // 2, 1)
            for k in range(2):
                start = pl.multiple_of(up_y[k] * (tile + margin), margin)
                strip = diag_in[2 * k + j][s].astype(F32)
                ext[2 * s, side, pl.ds(start, margin)] = strip
                ext[2 * s + 1, side, pl.ds(start, margin)] = pltpu.roll(strip, LANES // 2, 1)
    grad[...] = jnp.zeros(grad.shape, F32)
    acc[...] = jnp.zeros(acc.shape, F32)

    lanes = lane_ids(extent)

    def visit(slot):
        y = row_of[slot]
        x = col_of[slot] + margin
        side = lax.shift_right_logical(x, 7)
        off = x & (LANES - 1)
        upper = lanes >= off
        back = (LANES - off) & (LANES - 1)

        def window(p):
            v0 = ext[p, side, pl.ds(y, extent), :]
            v1 = ext[p, side + 1, pl.ds(y, extent), :]
            return pltpu.roll(jnp.where(upper, v0, v1), back, 1)

        def scatter(p, value):
            moved = pltpu.roll(value, off, 1)
            grad[p, side, pl.ds(y, extent), :] += jnp.where(upper, moved, 0.0)
            grad[p, side + 1, pl.ds(y, extent), :] += jnp.where(upper, 0.0, moved)

        p_tab, q_tab = first[...], second[...]
        prop = (kern[0], kern[1])
        waves = [(probe[m, 0], probe[m, 1]) for m in range(modes)]
        inputs = [waves]
        cells = []
        for s in range(slices):
            cells.append((window(2 * s), window(2 * s + 1)))
            exits = [cmul(w, cells[s]) for w in inputs[s]]
            far = transform(exits, p_tab, q_tab)
            if s + 1 < slices:
                inputs.append(transform([cmul(prop, f) for f in far], q_tab, p_tab))
        total = far[0][0] * far[0][0] + far[0][1] * far[0][1]
        for re, im in far[1:]:
            total = total + (re * re + im * im)
        scale = amp[slot].astype(F32) * lax.rsqrt(jnp.maximum(total, 0.25))
        factor = (1.0 - scale) * live_of[slot]
        back_waves = transform([(re * factor, im * factor) for re, im in far], q_tab, p_tab)
        for s in reversed(range(slices)):
            q_re, q_im = cmul_conj(inputs[s][0], back_waves[0])
            for m in range(1, modes):
                re, im = cmul_conj(inputs[s][m], back_waves[m])
                q_re, q_im = q_re + re, q_im + im
            scatter(2 * s, q_re)
            scatter(2 * s + 1, q_im)
            terms = [cmul_conj(cells[s], g) for g in back_waves]
            if s > 0:
                inner = transform(terms, p_tab, q_tab)
                back_waves = transform([cmul_conj(prop, f) for f in inner], q_tab, p_tab)
        for m in range(modes):
            acc[2 * m] += terms[m][0]
            acc[2 * m + 1] += terms[m][1]

    def body(i, carry):
        visit(i)
        return carry

    lax.fori_loop(0, (k_n + 1) * CAP, body, 0)

    per_chunk = probe_grad.shape[1]
    flat_rows = extent // per_chunk if per_chunk < extent else 1
    for q in range(2 * modes):
        value = acc[q].astype(BF16)
        for f in range(flat_rows):
            at = q * extent + f * per_chunk if flat_rows > 1 else q * extent
            width = per_chunk if flat_rows > 1 else extent
            probe_grad[at // per_chunk, at % per_chunk : at % per_chunk + width] = value[
                f * width : (f + 1) * width
            ]
    for k in range(2):
        start = pl.multiple_of(up_y[k] * (tile + margin), margin)
        for p in range(slices * 2):
            for t in range(tiles):
                ty_out[k][p * tiles + t] = grad[p, 1 + t, pl.ds(start, margin)].astype(BF16)
    for s in range(slices):
        for j in range(2):
            side = up_x[j] * (tiles + 1)
            re = grad[2 * s, side, margin : margin + tile]
            im = grad[2 * s + 1, side, margin : margin + tile]
            mask = half_mask(tile, 1 - up_x[j])
            tx_out[j][s] = jnp.where(mask, re, pltpu.roll(im, LANES // 2, 1)).astype(BF16)
            for k in range(2):
                start = pl.multiple_of(up_y[k] * (tile + margin), margin)
                re = grad[2 * s, side, pl.ds(start, margin)]
                im = grad[2 * s + 1, side, pl.ds(start, margin)]
                mask = half_mask(margin, 1 - up_x[j])
                diag_out[2 * k + j][s] = jnp.where(mask, re, pltpu.roll(im, LANES // 2, 1)).astype(BF16)


def update_kernel(obj, grad, probe, *refs):
    ty_in, tx_in, diag_in, out = refs[:2], refs[2:4], refs[4:8], refs[8]
    slices, tile, extent = obj.shape[0], obj.shape[2], probe.shape[2]
    margin, tiles = extent // 2, obj.shape[3] // LANES
    row, col = lax.axis_index("ty"), lax.axis_index("tx")
    up_y, up_x = ups(row), ups(col)
    power = jnp.sum(probe[...] * probe[...]) / (extent * extent)
    rate = jnp.full((1, 1), 1.0, F32) / (power + 1e-06)
    for p in range(slices * 2):
        for t in range(tiles):
            span = slice(t * LANES, (t + 1) * LANES)
            piece = grad[p, 1 + t, margin : margin + tile]
            out[p // 2, p % 2, :, span] = obj[p // 2, p % 2, :, span] - piece * rate
    for p in range(slices * 2):
        for k in range(2):
            start = pl.multiple_of(up_y[k] * (tile - margin), margin)
            for t in range(tiles):
                span = slice(t * LANES, (t + 1) * LANES)
                out[p // 2, p % 2, pl.ds(start, margin), span] -= (
                    ty_in[k][p * tiles + t].astype(F32) * rate
                )
    for s in range(slices):
        for j in range(2):
            lane = pl.multiple_of(up_x[j] * (tile - LANES), LANES)
            strip = tx_in[j][s].astype(F32) * rate
            mask = half_mask(tile, up_x[j])
            out[s, 0, :, pl.ds(lane, LANES)] -= jnp.where(mask, strip, 0.0)
            out[s, 1, :, pl.ds(lane, LANES)] -= jnp.where(mask, pltpu.roll(strip, LANES // 2, 1), 0.0)
            for k in range(2):
                start = pl.multiple_of(up_y[k] * (tile - margin), margin)
                strip = diag_in[2 * k + j][s].astype(F32) * rate
                mask = half_mask(margin, up_x[j])
                out[s, 0, pl.ds(start, margin), pl.ds(lane, LANES)] -= jnp.where(mask, strip, 0.0)
                out[s, 1, pl.ds(start, margin), pl.ds(lane, LANES)] -= jnp.where(
                    mask, pltpu.roll(strip, LANES // 2, 1), 0.0
                )


def sum_kernel(sizes, own, *refs):
    rounds = sizes[2]
    parts, out, held = refs[: len(rounds)], refs[len(rounds)], refs[len(rounds) + 1]
    row = lax.axis_index("ty")
    held[row] = own[...]
    for k, partner in enumerate(rounds):
        held[pick(row, partner)] = parts[k][...]
    total = held[0]
    for i in range(1, held.shape[0]):
        total = total + held[i]
    out[...] = total.astype(out.dtype)


def probe_kernel(probe, gathered, out):
    modes, extent = probe.shape[0], probe.shape[2]
    summed = gathered[...].astype(F32)
    mean = jnp.sum(summed * summed) / summed.size
    rate = jnp.full((1, 1), 0.5, F32) * lax.rsqrt(jnp.full((1, 1), 1.0, F32) * (mean + 1e-06))
    for m in range(modes):
        for c in range(2):
            at = (2 * m + c) * extent
            out[m, c] = probe[m, c] - gathered[at : at + extent].astype(F32) * rate


VMEM = pl.BlockSpec(memory_space=pltpu.VMEM)
SMEM = pl.BlockSpec(memory_space=pltpu.SMEM)


def call(kernel, name, operands, specs, outs, scratch=()):
    return pl.pallas_call(
        kernel,
        out_shape=outs,
        in_specs=specs,
        out_specs=[VMEM] * len(outs) if isinstance(outs, (list, tuple)) else VMEM,
        scratch_shapes=list(scratch),
        compiler_params=pltpu.CompilerParams(vmem_limit_bytes=56 * 1024 * 1024),
        name=name,
    )(*operands)


def swap(value, axis, side):
    return lax.ppermute(value, axis, neighbour_pairs(side, lax.axis_size(axis)))


def swap_diagonal(value, side_y, side_x):
    n_ty, n_tx = lax.axis_size("ty"), lax.axis_size("tx")
    pairs = [
        (y0 * n_tx + x0, y1 * n_tx + x1)
        for y0, y1 in neighbour_pairs(side_y, n_ty)
        for x0, x1 in neighbour_pairs(side_x, n_tx)
    ]
    return lax.ppermute(value, ("ty", "tx"), pairs)


def on_device(object_slices, probe_modes, patterns, positions, counts):
    slices, _, tile, _ = object_slices.shape
    modes, _, extent, _ = probe_modes.shape
    margin, tiles = extent // 2, tile // LANES
    n_ty, n_tx = lax.axis_size("ty"), lax.axis_size("tx")
    rounds = pairings(n_ty)
    sizes = (n_ty, n_tx, rounds)
    parts = slices * 2 * tiles
    struct = jax.ShapeDtypeStruct
    strips = [struct((slices, tile, LANES), BF16)] * 2
    corners = [struct((slices, margin, LANES), BF16)] * 4
    k_n = len(rounds)
    packed = call(
        lambda *r: pack_kernel(sizes, *r),
        "pack",
        (object_slices, patterns, positions, counts),
        [VMEM, VMEM, SMEM, SMEM],
        [struct(((parts if k < 2 else 0) + 2 * CAP, margin, LANES), BF16) for k in range(k_n)]
        + strips
        + corners,
    )
    ty_in = [
        lax.ppermute(packed[k], "ty", [(i, rounds[k][i]) for i in range(n_ty)]) for k in range(k_n)
    ]
    tx_in = [swap(packed[k_n + j], "tx", j) for j in range(2)]
    diag_in = [swap_diagonal(packed[k_n + 2 + q], q // 2, q % 2) for q in range(4)]

    first, second, kern = make_tables(extent)
    slots = (k_n + 1) * CAP
    ext_shape = (slices * 2, tiles + 2, tile + extent, LANES)
    chunk = modes * 2 * extent // n_tx
    results = call(
        lambda *r: main_kernel(sizes, *r),
        "patterns",
        (object_slices, patterns, positions, counts, probe_modes, first, second, kern)
        + tuple(ty_in + tx_in + diag_in),
        [VMEM, VMEM, SMEM, SMEM] + [VMEM] * (4 + k_n + 6),
        [struct(ext_shape, F32), struct((n_tx, chunk, LANES), BF16)]
        + [struct((parts, margin, LANES), BF16)] * 2
        + strips
        + corners,
        [
            pltpu.VMEM(ext_shape, F32),
            pltpu.VMEM((slots, extent, extent), BF16),
            pltpu.VMEM((2 * modes, extent, extent), F32),
            pltpu.SMEM((slots,), jnp.int32),
            pltpu.SMEM((slots,), jnp.int32),
            pltpu.SMEM((slots,), F32),
        ],
    )
    grad, probe_grad = results[0], results[1]
    ty_back = [swap(results[2 + k], "ty", k) for k in range(2)]
    tx_back = [swap(results[4 + j], "tx", j) for j in range(2)]
    diag_back = [swap_diagonal(results[6 + q], q // 2, q % 2) for q in range(4)]

    shares = lax.all_to_all(probe_grad, "tx", split_axis=0, concat_axis=0, tiled=True)
    mine = jnp.sum(shares.astype(F32), axis=0)
    others = [
        lax.ppermute(mine, "ty", [(i, rounds[k][i]) for i in range(n_ty)]) for k in range(k_n)
    ]
    full = call(
        lambda *r: sum_kernel(sizes, *r),
        "sum_rows",
        tuple([mine] + others),
        [VMEM] * (k_n + 1),
        struct((chunk, LANES), BF16),
        [pltpu.VMEM((n_ty, chunk, LANES), F32)],
    )
    gathered = lax.all_gather(full, "tx", axis=0, tiled=True)
    new_object = call(
        update_kernel,
        "update",
        (object_slices, grad, probe_modes) + tuple(ty_back + tx_back + diag_back),
        [VMEM] * 11,
        struct(object_slices.shape, F32),
    )
    new_probe = call(
        probe_kernel,
        "probe",
        (probe_modes, gathered),
        [VMEM] * 2,
        struct(probe_modes.shape, F32),
    )
    return (new_object, new_probe)


def solution(mesh):
    return jax.shard_map(
        on_device,
        mesh=mesh,
        in_specs=(P(None, None, "ty", "tx"), P(), P(("ty", "tx"), None, None), P(), P()),
        out_specs=(P(None, None, "ty", "tx"), P()),
        check_vma=False,
    )
```

```python
import math

import numpy as np
import jax
import jax.numpy as jnp
from jax import lax
from jax.experimental import pallas as pl
from jax.experimental.pallas import tpu as pltpu
from jax.sharding import PartitionSpec as P


CAP = 2
PROPAGATION = 0.37
LANES = 128
BF16 = jnp.bfloat16
F32 = jnp.float32


def make_tables(extent):
    indices = np.arange(extent, dtype=np.int32)
    product = indices[:, None] * indices[None, :] % extent
    angles = np.float32(2.0 * math.pi / extent) * product.astype(np.float32)
    norm_scale = np.float32(1.0 / math.sqrt(extent))
    real_table = jnp.asarray(np.cos(angles) * norm_scale, F32).astype(BF16)
    imag_table = jnp.asarray(-np.sin(angles) * norm_scale, F32).astype(BF16)
    first = jnp.concatenate(
        [
            jnp.concatenate([real_table, imag_table], 1),
            jnp.concatenate([-imag_table, real_table], 1),
        ],
        0,
    )
    second = jnp.concatenate(
        [
            jnp.concatenate([real_table, -imag_table], 1),
            jnp.concatenate([imag_table, real_table], 1),
        ],
        0,
    )
    frequency = np.where(indices < extent // 2, indices, indices - extent).astype(np.float32)
    phases = np.float32(-math.pi * PROPAGATION / extent) * (
        frequency[:, None] ** 2 + frequency[None, :] ** 2
    )
    kernel = jnp.asarray(np.stack([np.cos(phases), np.sin(phases)]), F32)
    return first, second, kernel


def pairings(n):
    if n == 2:
        return [[1, 0]]
    assert n % 2 == 0 and all((n - 1) % d for d in range(2, n - 1))
    odd = n - 1
    rounds = []
    for k in range(odd):
        partner = [0] * n
        partner[odd], partner[k] = k, odd
        for i in range(1, n // 2):
            a, b = (k + i) % odd, (k - i) % odd
            partner[a], partner[b] = b, a
        rounds.append(partner)
    order = [odd]
    while len(order) < n:
        order.append(rounds[(len(order) - 1) % 2][order[-1]])
    label = {v: i for i, v in enumerate(order)}
    return [[label[r[order[i]]] for i in range(n)] for r in rounds]


def neighbour(side, i):
    return 1 if (i + side) % 2 == 0 else -1


def neighbour_pairs(side, n):
    steps = [(i, i + neighbour(side, i)) for i in range(n)]
    return [(i, j) for i, j in steps if 0 <= j < n]


def pick(index, values):
    chosen = jnp.int32(values[0])
    for i in range(1, len(values)):
        chosen = jnp.where(index == i, jnp.int32(values[i]), chosen)
    return chosen


def lane_ids(rows):
    return lax.broadcasted_iota(jnp.int32, (rows, LANES), 1)


def half_mask(rows, upper):
    return (lane_ids(rows) >= LANES // 2).astype(jnp.int32) == upper


def ups(index):
    even = 1 - lax.rem(index, 2)
    return [even, 1 - even]


def slot_scan(pos, cnt, sizes, source, col, per_device, low, height):
    n_tx = sizes[1]
    base = (source * n_tx + col) * per_device
    count = cnt[source * n_tx + col]
    zero = jnp.int32(0)
    found, ys, xs, lives = [zero] * CAP, [zero] * CAP, [zero] * CAP, [zero] * CAP
    seen = zero
    for i in range(per_device):
        y, x = pos[0, base + i], pos[1, base + i]
        hit = (i < count) & (y >= low) & (y < low + height)
        for c in range(CAP):
            this = hit & (seen == c)
            found[c] = jnp.where(this, i, found[c])
            ys[c] = jnp.where(this, y - low, ys[c])
            xs[c] = jnp.where(this, x, xs[c])
            lives[c] = jnp.where(this, 1, lives[c])
        seen = seen + hit.astype(jnp.int32)
    return found, ys, xs, lives


def rows_kernel(sizes, obj, pat, pos, cnt, ty_a, ty_b, held, rows, sems):
    planes, tile, margin = obj.shape[0] * 2, obj.shape[2], rows.shape[3]
    tiles = obj.shape[3] // LANES
    row, col = lax.axis_index("ty"), lax.axis_index("tx")
    up_y = ups(row)
    copies = [pltpu.make_async_copy(pat, held, sems.at[2])]
    for k in range(2):
        start = pl.multiple_of(up_y[k] * (tile - margin), margin)
        copies.append(pltpu.make_async_copy(obj.at[:, :, pl.ds(start, margin), :], rows.at[k], sems.at[k]))
    for copy in copies:
        copy.start()
    target = pick(row, sizes[2][0]) * tile
    found = slot_scan(pos, cnt, sizes, row, col, pat.shape[0], target, tile)[0]
    copies[0].wait()
    for c in range(CAP):
        for h in range(2):
            ty_a[planes * tiles + 2 * c + h] = held[found[c], h * margin : (h + 1) * margin, :]
    for k, out in enumerate((ty_a, ty_b)):
        copies[1 + k].wait()
        for p in range(planes):
            for t in range(tiles):
                block = rows[k, p // 2, p % 2, :, t * LANES : (t + 1) * LANES]
                out[p * tiles + t] = block.astype(BF16)


def columns_kernel(obj, tx_a, tx_b):
    slices, tile = obj.shape[0], obj.shape[2]
    up_x = ups(lax.axis_index("tx"))
    for j, out in enumerate((tx_a, tx_b)):
        lane = pl.ds(pl.multiple_of(up_x[j] * (tile - LANES), LANES), LANES)
        for s in range(slices):
            re, im = obj[s, 0, :, lane], obj[s, 1, :, lane]
            packed = jnp.where(half_mask(tile, up_x[j]), re, pltpu.roll(im, LANES // 2, 1))
            out[s] = packed.astype(BF16)


def tile_kernel(sizes, obj, pat, pos, cnt, ext, grad, *routed):
    rounds = sizes[2]
    slices, tile = obj.shape[0], obj.shape[2]
    tiles = obj.shape[3] // LANES
    margin = (ext.shape[2] - tile) // 2
    row, col = lax.axis_index("ty"), lax.axis_index("tx")
    targets = [pick(row, partner) * tile for partner in rounds[1:]]
    found = [slot_scan(pos, cnt, sizes, row, col, pat.shape[0], t, tile)[0] for t in targets]
    for k, out in enumerate(routed):
        for c in range(CAP):
            out[c] = pat[found[k][c]]
    for p in range(slices * 2):
        for t in range(tiles):
            ext[p, 1 + t, margin : margin + tile] = obj[p // 2, p % 2, :, t * LANES : (t + 1) * LANES]
    grad[...] = jnp.zeros(grad.shape, F32)


def corner_kernel(slices, tiles, ty_a, ty_b, out_a, out_b):
    up_x = ups(lax.axis_index("tx"))
    for j, out in enumerate((out_a, out_b)):
        at = up_x[j] * (tiles - 1)
        for k, rows in enumerate((ty_a, ty_b)):
            for s in range(slices):
                re = rows[2 * s * tiles + at].astype(F32)
                im = rows[(2 * s + 1) * tiles + at].astype(F32)
                packed = jnp.where(half_mask(re.shape[0], up_x[j]), re, pltpu.roll(im, LANES // 2, 1))
                out[k * slices + s] = packed.astype(BF16)


def cmul(a, b):
    return a[0] * b[0] - a[1] * b[1], a[0] * b[1] + a[1] * b[0]


def cmul_conj(a, b):
    return a[0] * b[0] + a[1] * b[1], a[0] * b[1] - a[1] * b[0]


def transform(fields, right, left):
    extent = fields[0][0].shape[0]
    joined = jnp.concatenate([jnp.concatenate([re, im], 1) for re, im in fields], 0).astype(BF16)
    half = jnp.dot(joined, right, preferred_element_type=F32).astype(BF16)
    blocks = []
    for m in range(len(fields)):
        part = half[m * extent : (m + 1) * extent]
        blocks.append(jnp.concatenate([part[:, :extent], part[:, extent:]], 0))
    whole = jnp.dot(left, jnp.concatenate(blocks, 1), preferred_element_type=F32)
    return [
        (whole[:extent, m * extent : (m + 1) * extent], whole[extent:, m * extent : (m + 1) * extent])
        for m in range(len(fields))
    ]


def find_slots(sizes, pos, cnt, per_device, tile, row_of, col_of, live_of):
    rounds = sizes[2]
    row, col = lax.axis_index("ty"), lax.axis_index("tx")
    own = None
    for k in range(len(rounds) + 1):
        source = row if k == 0 else pick(row, rounds[k - 1])
        found, ys, xs, lives = slot_scan(pos, cnt, sizes, source, col, per_device, row * tile, tile)
        own = found if k == 0 else own
        for c in range(CAP):
            slot = k * CAP + c
            row_of[slot] = ys[c]
            col_of[slot] = jnp.where(lives[c] == 1, xs[c] - col * tile, 0)
            if live_of is not None:
                live_of[slot] = lives[c].astype(F32)
    return own


def places(row_of, col_of, slot, margin, lanes):
    x = col_of[slot] + margin
    off = x & (LANES - 1)
    return row_of[slot], lax.shift_right_logical(x, 7), off, lanes >= off


def window(ext, place, p):
    y, side, off, upper = place
    v0 = ext[p, side, pl.ds(y, LANES), :]
    v1 = ext[p, side + 1, pl.ds(y, LANES), :]
    return pltpu.roll(jnp.where(upper, v0, v1), (LANES - off) & (LANES - 1), 1)


def forward_kernel(sizes, per_device, pos, cnt, probe, *refs):
    sources, refs = refs[:3], refs[3:]
    ty_in, tx_in, corner_in = refs[:2], refs[2:4], refs[4:6]
    ext, psi, waves, first, second, kern, row_of, col_of, sems = refs[7:]
    copies = [
        pltpu.make_async_copy(a, b, sems.at[i])
        for i, (a, b) in enumerate(zip(sources, (first, second, kern)))
    ]
    for copy in copies:
        copy.start()
    modes, extent = probe.shape[0], probe.shape[2]
    planes, margin, tiles = ext.shape[0], extent // 2, ext.shape[1] - 2
    slices, tile = planes // 2, ext.shape[2] - extent
    up_y, up_x = ups(lax.axis_index("ty")), ups(lax.axis_index("tx"))
    find_slots(sizes, pos, cnt, per_device, tile, row_of, col_of, None)
    for k in range(2):
        rows = pl.ds(pl.multiple_of(up_y[k] * (tile + margin), margin), margin)
        for p in range(planes):
            for t in range(tiles):
                ext[p, 1 + t, rows] = ty_in[k][p * tiles + t].astype(F32)
        for s in range(slices):
            for j in range(2):
                side = up_x[j] * (tiles + 1)
                strip = corner_in[j][k * slices + s].astype(F32)
                ext[2 * s, side, rows] = strip
                ext[2 * s + 1, side, rows] = pltpu.roll(strip, LANES // 2, 1)
    for s in range(slices):
        for j in range(2):
            side = up_x[j] * (tiles + 1)
            strip = tx_in[j][s].astype(F32)
            ext[2 * s, side, margin : margin + tile] = strip
            ext[2 * s + 1, side, margin : margin + tile] = pltpu.roll(strip, LANES // 2, 1)
    lanes = lane_ids(extent)
    for copy in copies:
        copy.wait()

    def body(i, carry):
        slots = [i * BATCH + b for b in range(BATCH)]
        p_tab, q_tab = first[...], second[...]
        prop = (kern[0], kern[1])
        where = [places(row_of, col_of, slot, margin, lanes) for slot in slots]
        fields = [(probe[m, 0], probe[m, 1]) for m in range(modes)] * BATCH
        for s in range(slices):
            cells = [(window(ext, w, 2 * s), window(ext, w, 2 * s + 1)) for w in where]
            exits = [cmul(w, cells[n // modes]) for n, w in enumerate(fields)]
            far_field = transform(exits, p_tab, q_tab)
            if s + 1 < slices:
                fields = transform([cmul(prop, f) for f in far_field], q_tab, p_tab)
            kept = fields if s + 1 < slices else far_field
            for n, (re, im) in enumerate(kept):
                at = 2 * (n % modes)
                if s + 1 < slices:
                    waves[s, slots[n // modes], at] = re
                    waves[s, slots[n // modes], at + 1] = im
                else:
                    psi[slots[n // modes], at] = re
                    psi[slots[n // modes], at + 1] = im
        return carry

    lax.fori_loop(0, psi.shape[0] // BATCH, body, 0)


def backward_kernel(sizes, pat, pos, cnt, probe, first, second, kern, ext, psi, waves, *refs):
    _, n_tx, rounds = sizes
    k_n = len(rounds)
    pat_in, refs = refs[:k_n], refs[k_n + 1 :]
    grad, ty_out, keep, share = refs[0], refs[1:3], refs[3], refs[4]
    amp, acc, row_of, col_of, live_of = refs[5:]
    modes, extent = probe.shape[0], probe.shape[2]
    planes, margin, tiles = ext.shape[0], extent // 2, ext.shape[1] - 2
    slices, tile = planes // 2, ext.shape[2] - extent
    parts = planes * tiles
    row, col = lax.axis_index("ty"), lax.axis_index("tx")
    up_y, up_x = ups(row), ups(col)
    start_y = [pl.multiple_of(up_y[k] * (tile + margin), margin) for k in range(2)]
    own = find_slots(sizes, pos, cnt, pat.shape[0], tile, row_of, col_of, live_of)
    for c in range(CAP):
        amp[c] = pat[own[c]]
        for h in range(2):
            amp[CAP + c, h * margin : (h + 1) * margin] = pat_in[0][parts + 2 * c + h]
        for k in range(1, k_n):
            amp[(k + 1) * CAP + c] = pat_in[k][c]
    acc[...] = jnp.zeros(acc.shape, F32)
    lanes = lane_ids(extent)

    def scatter(place, p, value):
        y, side, off, upper = place
        moved = pltpu.roll(value, off, 1)
        grad[p, side, pl.ds(y, extent), :] += jnp.where(upper, moved, 0.0)
        grad[p, side + 1, pl.ds(y, extent), :] += jnp.where(upper, 0.0, moved)

    def body(i, carry):
        slots = [i * BATCH + b for b in range(BATCH)]
        p_tab, q_tab = first[...], second[...]
        prop = (kern[0], kern[1])
        where = [places(row_of, col_of, slot, margin, lanes) for slot in slots]
        residues = []
        for slot in slots:
            mine = [(psi[slot, 2 * m], psi[slot, 2 * m + 1]) for m in range(modes)]
            total = mine[0][0] * mine[0][0] + mine[0][1] * mine[0][1]
            for re, im in mine[1:]:
                total = total + (re * re + im * im)
            scale = amp[slot].astype(F32) * lax.rsqrt(jnp.maximum(total, 0.25))
            factor = (1.0 - scale) * live_of[slot]
            residues += [(re * factor, im * factor) for re, im in mine]
        back_waves = transform(residues, q_tab, p_tab)
        for s in reversed(range(slices)):
            for n, slot in enumerate(slots):
                for m in range(modes):
                    if s == 0:
                        wave = (probe[m, 0], probe[m, 1])
                    else:
                        wave = (waves[s - 1, slot, 2 * m], waves[s - 1, slot, 2 * m + 1])
                    re, im = cmul_conj(wave, back_waves[n * modes + m])
                    q_re, q_im = (re, im) if m == 0 else (q_re + re, q_im + im)
                scatter(where[n], 2 * s, q_re)
                scatter(where[n], 2 * s + 1, q_im)
            cells = [(window(ext, w, 2 * s), window(ext, w, 2 * s + 1)) for w in where]
            terms = [cmul_conj(cells[n // modes], g) for n, g in enumerate(back_waves)]
            if s > 0:
                inner = transform(terms, p_tab, q_tab)
                back_waves = transform([cmul_conj(prop, f) for f in inner], q_tab, p_tab)
        for m in range(modes):
            for c in range(2):
                value = terms[m][c]
                for n in range(1, BATCH):
                    value = value + terms[n * modes + m][c]
                acc[2 * m + c] += value
        return carry

    lax.fori_loop(0, psi.shape[0] // BATCH, body, 0)

    chunk = keep.shape[1]
    core = lax.rem(col, 2)
    for i in range(n_tx // 2):
        for out, parity in ((keep, core), (share, 1 - core)):
            at = (2 * i + parity) * chunk
            index = lax.div(at, extent)
            inside = pl.multiple_of(at - index * extent, chunk)
            out[i] = acc[index, pl.ds(inside, chunk), :]
    for k in range(2):
        for p in range(planes):
            for t in range(tiles):
                ty_out[k][p * tiles + t] = grad[p, 1 + t, pl.ds(start_y[k], margin)].astype(BF16)
        for j in range(2):
            side, mask = up_x[j] * (tiles + 1), half_mask(margin, 1 - up_x[j])
            for s in range(slices):
                re = grad[2 * s, side, pl.ds(start_y[k], margin)]
                im = grad[2 * s + 1, side, pl.ds(start_y[k], margin)]
                packed = jnp.where(mask, re, pltpu.roll(im, LANES // 2, 1))
                ty_out[k][parts + j * slices + s] = packed.astype(BF16)


def pair_kernel(keep, share, own, *outs):
    at = lax.shift_right_logical(lax.axis_index("tx"), 1)
    own[...] = keep[at] + share[at]
    for k, out in enumerate(outs, 1):
        other = jnp.bitwise_xor(at, k)
        out[...] = (keep[other] + share[other]).astype(BF16)


def join_kernel(*refs):
    parts, out = refs[:-1], refs[-1]
    at = lax.shift_right_logical(lax.axis_index("tx"), 1)
    for k, part in enumerate(parts):
        out[jnp.bitwise_xor(at, k)] = part[...]


def share_kernel(own, *refs):
    parts, out = refs[:-1], refs[-1]
    total = own[...]
    for part in parts:
        total = total + part[...].astype(F32)
    out[...] = total.astype(out.dtype)


def update_rate(probe):
    extent = probe.shape[2]
    power = jnp.sum(probe[...] * probe[...]) / (extent * extent)
    return jnp.full((1, 1), 1.0, F32) / (power + 1e-06)


def fold_kernel(tile, old, ty_a, ty_b, tx_a, tx_b, grad):
    planes, tiles = grad.shape[0], grad.shape[1] - 2
    slices, margin = planes // 2, (grad.shape[2] - tile) // 2
    up_y, up_x = ups(lax.axis_index("ty")), ups(lax.axis_index("tx"))
    for k, strips in enumerate((ty_a, ty_b)):
        rows = pl.ds(pl.multiple_of(margin + up_y[k] * (tile - margin), margin), margin)
        for p in range(planes):
            for t in range(tiles):
                grad[p, 1 + t, rows] += strips[p * tiles + t].astype(F32)
        for j in range(2):
            side, mask = up_x[j] * (tiles + 1), half_mask(margin, 1 - up_x[j])
            for s in range(slices):
                strip = strips[planes * tiles + j * slices + s].astype(F32)
                grad[2 * s, side, rows] += jnp.where(mask, strip, 0.0)
                grad[2 * s + 1, side, rows] += jnp.where(mask, pltpu.roll(strip, LANES // 2, 1), 0.0)
    inner = slice(margin, margin + tile)
    for j, out in enumerate((tx_a, tx_b)):
        side, mask = up_x[j] * (tiles + 1), half_mask(tile, 1 - up_x[j])
        for s in range(slices):
            re, im = grad[2 * s, side, inner], grad[2 * s + 1, side, inner]
            out[s] = jnp.where(mask, re, pltpu.roll(im, LANES // 2, 1)).astype(BF16)


def middle_kernel(obj, grad, probe, out, fresh, sems):
    tile, tiles = obj.shape[2], obj.shape[3] // LANES
    margin = (grad.shape[2] - tile) // 2
    rate = update_rate(probe)
    copies = []
    for p in range(obj.shape[0] * 2):
        s, c = p // 2, p % 2
        for t in range(1, tiles - 1):
            piece = obj[s, c, :, t * LANES : (t + 1) * LANES] - grad[p, 1 + t, margin : margin + tile] * rate
            fresh[s, c, :, (t - 1) * LANES : t * LANES] = piece
        copies.append(
            pltpu.make_async_copy(
                fresh.at[s, c], out.at[s, c, :, LANES : (tiles - 1) * LANES], sems.at[p]
            )
        )
        copies[-1].start()
    for copy in copies:
        copy.wait()


def edges_kernel(obj, grad, tx_a, tx_b, probe, old, out, fresh, sems):
    slices, tile, tiles = obj.shape[0], obj.shape[2], obj.shape[3] // LANES
    margin = (grad.shape[2] - tile) // 2
    up_x = ups(lax.axis_index("tx"))
    rate = update_rate(probe)
    copies = []
    for high in range(2):
        t, mask = high * (tiles - 1), half_mask(tile, high)
        span = slice(t * LANES, (t + 1) * LANES)
        for s in range(slices):
            strip = jnp.where(up_x[0] == high, tx_a[s].astype(F32), tx_b[s].astype(F32))
            for c in range(2):
                if c == 1:
                    strip = pltpu.roll(strip, LANES // 2, 1)
                total = grad[2 * s + c, 1 + t, margin : margin + tile] + jnp.where(mask, strip, 0.0)
                fresh[high, s, c] = obj[s, c, :, span] - total * rate
            copies.append(
                pltpu.make_async_copy(fresh.at[high, s], out.at[s, :, :, span], sems.at[high * slices + s])
            )
            copies[-1].start()
    for copy in copies:
        copy.wait()


def probe_kernel(probe, joined, other, out, held):
    modes, extent, chunk = probe.shape[0], probe.shape[2], joined.shape[1]
    core = lax.rem(lax.axis_index("tx"), 2)
    for i in range(joined.shape[0]):
        for part, parity in ((joined, core), (other, 1 - core)):
            at = pl.multiple_of((2 * i + parity) * chunk, chunk)
            held[pl.ds(at, chunk), :] = part[i].astype(F32)
    summed = held[...]
    mean = jnp.sum(summed * summed) / summed.size
    step = jnp.full((1, 1), 0.5, F32) * lax.rsqrt(jnp.full((1, 1), 1.0, F32) * (mean + 1e-06))
    for m in range(modes):
        for c in range(2):
            at = (2 * m + c) * extent
            out[m, c] = probe[m, c] - held[at : at + extent] * step


def sum_kernel(sizes, own, *refs):
    rounds = sizes[2]
    parts, out, held = refs[: len(rounds)], refs[len(rounds)], refs[len(rounds) + 1]
    row = lax.axis_index("ty")
    held[row] = own[...].astype(F32)
    for k, partner in enumerate(rounds):
        held[pick(row, partner)] = parts[k][...].astype(F32)
    total = held[0]
    for i in range(1, held.shape[0]):
        total = total + held[i]
    out[...] = total.astype(out.dtype)


BATCH = 4
VMEM_BYTES = 10 * 1024 * 1024
VMEM = pl.BlockSpec(memory_space=pltpu.VMEM)
SMEM = pl.BlockSpec(memory_space=pltpu.SMEM)
ANY = pl.BlockSpec(memory_space=pl.ANY)


def call(kernel, operands, specs, outs, scratch=(), aliases=None, out_specs=None):
    single = not isinstance(outs, (list, tuple))
    return pl.pallas_call(
        kernel,
        out_shape=outs,
        in_specs=specs,
        out_specs=out_specs or (VMEM if single else [VMEM] * len(outs)),
        scratch_shapes=list(scratch),
        input_output_aliases=aliases or {},
        compiler_params=pltpu.CompilerParams(vmem_limit_bytes=VMEM_BYTES),
    )(*operands)


def near(value):
    return pltpu.with_memory_space_constraint(value, pltpu.VMEM)


def far(value):
    return pltpu.with_memory_space_constraint(value, pltpu.HBM)


def send(value, axis, pairs):
    return near(lax.ppermute(value, axis, pairs))


def step(object_slices, probe_modes, patterns, positions, counts):
    slices, _, tile, _ = object_slices.shape
    modes, _, extent, _ = probe_modes.shape
    margin, tiles = extent // 2, tile // LANES
    n_ty, n_tx = lax.axis_size("ty"), lax.axis_size("tx")
    rounds = pairings(n_ty)
    sizes = (n_ty, n_tx, rounds)
    parts = slices * 2 * tiles
    k_n = len(rounds)
    places = positions.T
    planes = slices * 2
    block = (margin, LANES)
    strips = [pltpu.VMEM((slices, tile, LANES), BF16)] * 2
    strips = [pltpu.VMEM((slices, tile, LANES), BF16)] * 2
    rows_out = [pltpu.VMEM((parts + 2 * slices,) + block, BF16)] * 2
    ty_a, ty_b, near_patterns = call(
        lambda *r: rows_kernel(sizes, *r),
        (far(object_slices), far(patterns), far(places), far(counts)),
        [ANY, ANY, SMEM, SMEM],
        [pltpu.VMEM((parts + extra,) + block, BF16) for extra in (2 * CAP, 0)]
        + [pltpu.VMEM(patterns.shape, BF16)],
        [pltpu.VMEM((2, slices, 2, margin, tile), F32), pltpu.SemaphoreType.DMA((3,))],
    )
    near_object, near_patterns = near(object_slices), near(near_patterns)
    tx_a, tx_b = call(columns_kernel, (near_object,), [VMEM], strips)

    def pair_rows(value, k):
        return send(value, "ty", [(i, rounds[k][i]) for i in range(n_ty)])

    def swap(value, axis, side):
        return send(value, axis, neighbour_pairs(side, lax.axis_size(axis)))

    def cross(value, k):
        return send(value, "tx", [(i, i ^ k) for i in range(n_tx)])

    ext_shape = (planes, tiles + 2, tile + extent, LANES)
    ty_in = [swap(ty_a, "ty", 0), swap(ty_b, "ty", 1)]
    tx_in = [swap(tx_a, "tx", 0), swap(tx_b, "tx", 1)]
    ext, grad, *routed = call(
        lambda *r: tile_kernel(sizes, *r),
        (near_object, near_patterns, far(places), far(counts)),
        [VMEM, VMEM, SMEM, SMEM],
        [pltpu.VMEM(ext_shape, F32)] * 2 + [pltpu.VMEM((CAP, extent, extent), BF16)] * (k_n - 1),
    )
    corners = call(
        lambda *r: corner_kernel(slices, tiles, *r),
        tuple(ty_in),
        [VMEM] * 2,
        [pltpu.VMEM((2 * slices,) + block, BF16)] * 2,
    )
    corner_in = [swap(corners[j], "tx", j) for j in range(2)]
    pat_in = [ty_in[0]] + [pair_rows(routed[k - 1], k) for k in range(1, k_n)]

    first, second, kern = make_tables(extent)
    slots = (k_n + 1) * CAP
    chunk = modes * 2 * extent // n_tx
    constants = (first, second, kern)
    field = (slots, 2 * modes, extent, extent)
    tables = [pltpu.SMEM((slots,), jnp.int32)] * 2
    ext, psi, waves, *constants = call(
        lambda *r: forward_kernel(sizes, patterns.shape[0], *r),
        (places, counts, near(probe_modes))
        + tuple(far(c) for c in constants)
        + tuple(ty_in + tx_in + corner_in)
        + (near(ext),),
        [SMEM, SMEM, VMEM] + [ANY] * 3 + [VMEM] * 7,
        [pltpu.VMEM(ext_shape, F32), pltpu.VMEM(field, F32), pltpu.VMEM((slices - 1,) + field, F32)]
        + [pltpu.VMEM(c.shape, c.dtype) for c in constants],
        tables + [pltpu.SemaphoreType.DMA((3,))],
        {12: 0},
    )
    results = call(
        lambda *r: backward_kernel(sizes, *r),
        (near_patterns, places, counts, near(probe_modes))
        + tuple(near(c) for c in constants)
        + (near(ext), near(psi), near(waves), *pat_in, near(grad)),
        [VMEM, SMEM, SMEM] + [VMEM] * (7 + k_n + 1),
        [pltpu.VMEM(ext_shape, F32)]
        + rows_out
        + [pltpu.VMEM((n_tx // 2, chunk, LANES), F32)] * 2,
        [pltpu.VMEM((slots, extent, extent), BF16), pltpu.VMEM((2 * modes, extent, extent), F32)]
        + tables
        + [pltpu.SMEM((slots,), F32)],
        {10 + k_n: 0},
    )
    grad, ty_a, ty_b, keep, share = results
    ty_back = [swap(ty_a, "ty", 0), swap(ty_b, "ty", 1)]
    mine, *shares = call(
        pair_kernel,
        (near(keep), cross(share, 1)),
        [VMEM] * 2,
        [pltpu.VMEM((chunk, LANES), F32)] + [pltpu.VMEM((chunk, LANES), BF16)] * (n_tx // 2 - 1),
    )
    others = tuple(cross(shares[k - 1], 2 * k) for k in range(1, n_tx // 2))
    mine = call(
        share_kernel, (near(mine),) + others, [VMEM] * (n_tx // 2), pltpu.VMEM((chunk, LANES), BF16)
    )
    rows_in = tuple(pair_rows(mine, k) for k in range(k_n))
    tx_a, tx_b, grad = call(
        lambda *r: fold_kernel(tile, *r),
        (near(grad), *ty_back),
        [VMEM] * 3,
        strips + [pltpu.VMEM(ext_shape, F32)],
        (),
        {0: 2},
    )
    tx_back = [swap(tx_a, "tx", 0), swap(tx_b, "tx", 1)]
    full = call(
        lambda *r: sum_kernel(sizes, *r),
        (near(mine),) + rows_in,
        [VMEM] * (k_n + 1),
        pltpu.VMEM((chunk, LANES), BF16),
        [pltpu.VMEM((n_ty, chunk, LANES), F32)],
    )
    gathered = tuple(cross(full, 2 * k) for k in range(1, n_tx // 2))
    joined = call(
        join_kernel,
        (near(full),) + gathered,
        [VMEM] * (n_tx // 2),
        pltpu.VMEM((n_tx // 2, chunk, LANES), BF16),
    )
    other = cross(joined, 1)
    partial = call(
        middle_kernel,
        (near_object, near(grad), near(probe_modes)),
        [VMEM] * 3,
        pltpu.HBM(object_slices.shape, F32),
        [pltpu.VMEM((slices, 2, tile, tile - 2 * LANES), F32), pltpu.SemaphoreType.DMA((planes,))],
        None,
        ANY,
    )
    new_object = call(
        edges_kernel,
        (near_object, near(grad), *tx_back, near(probe_modes), far(partial)),
        [VMEM] * 5 + [ANY],
        pltpu.HBM(object_slices.shape, F32),
        [
            pltpu.VMEM((2, slices, 2, tile, LANES), F32),
            pltpu.SemaphoreType.DMA((2 * slices,)),
        ],
        {5: 0},
        ANY,
    )
    new_probe = call(
        probe_kernel,
        (near(probe_modes), near(joined), other),
        [VMEM] * 3,
        jax.ShapeDtypeStruct(probe_modes.shape, F32),
        [pltpu.VMEM((modes * 2 * extent, LANES), F32)],
    )
    return (new_object, new_probe)


def solution(mesh):
    return jax.shard_map(
        step,
        mesh=mesh,
        in_specs=(P(None, None, "ty", "tx"), P(), P(("ty", "tx"), None, None), P(), P()),
        out_specs=(P(None, None, "ty", "tx"), P()),
        check_vma=False,
    )
```

```python
import math

import numpy as np
import jax
import jax.numpy as jnp
from jax import lax
from jax.experimental import pallas as pl
from jax.experimental.pallas import tpu as pltpu
from jax.sharding import PartitionSpec as P


CAP = 2
PROPAGATION = 0.37
LANES = 128
BF16 = jnp.bfloat16
F32 = jnp.float32


def make_tables(extent):
    indices = np.arange(extent, dtype=np.int32)
    product = indices[:, None] * indices[None, :] % extent
    angles = np.float32(2.0 * math.pi / extent) * product.astype(np.float32)
    norm_scale = np.float32(1.0 / math.sqrt(extent))
    real_table = jnp.asarray(np.cos(angles) * norm_scale, F32).astype(BF16)
    imag_table = jnp.asarray(-np.sin(angles) * norm_scale, F32).astype(BF16)
    first = jnp.concatenate(
        [
            jnp.concatenate([real_table, imag_table], 1),
            jnp.concatenate([-imag_table, real_table], 1),
        ],
        0,
    )
    second = jnp.concatenate(
        [
            jnp.concatenate([real_table, -imag_table], 1),
            jnp.concatenate([imag_table, real_table], 1),
        ],
        0,
    )
    frequency = np.where(indices < extent // 2, indices, indices - extent).astype(np.float32)
    phases = np.float32(-math.pi * PROPAGATION / extent) * (
        frequency[:, None] ** 2 + frequency[None, :] ** 2
    )
    kernel = jnp.asarray(np.stack([np.cos(phases), np.sin(phases)]), F32)
    return first, second, kernel


def pairings(n):
    if n == 2:
        return [[1, 0]]
    assert n % 2 == 0 and all((n - 1) % d for d in range(2, n - 1))
    odd = n - 1
    rounds = []
    for k in range(odd):
        partner = [0] * n
        partner[odd], partner[k] = k, odd
        for i in range(1, n // 2):
            a, b = (k + i) % odd, (k - i) % odd
            partner[a], partner[b] = b, a
        rounds.append(partner)
    order = [odd]
    while len(order) < n:
        order.append(rounds[(len(order) - 1) % 2][order[-1]])
    label = {v: i for i, v in enumerate(order)}
    return [[label[r[order[i]]] for i in range(n)] for r in rounds]


def neighbour(side, i):
    return 1 if (i + side) % 2 == 0 else -1


def neighbour_pairs(side, n):
    steps = [(i, i + neighbour(side, i)) for i in range(n)]
    return [(i, j) for i, j in steps if 0 <= j < n]


def pick(index, values):
    chosen = jnp.int32(values[0])
    for i in range(1, len(values)):
        chosen = jnp.where(index == i, jnp.int32(values[i]), chosen)
    return chosen


def lane_ids(rows):
    return lax.broadcasted_iota(jnp.int32, (rows, LANES), 1)


def half_mask(rows, upper):
    return (lane_ids(rows) >= LANES // 2).astype(jnp.int32) == upper


def ups(index):
    even = 1 - lax.rem(index, 2)
    return [even, 1 - even]


def slot_scan(pos, cnt, sizes, source, col, per_device, low, height):
    n_tx = sizes[1]
    base = (source * n_tx + col) * per_device
    count = cnt[source * n_tx + col]
    zero = jnp.int32(0)
    found, ys, xs, lives = [zero] * CAP, [zero] * CAP, [zero] * CAP, [zero] * CAP
    seen = zero
    for i in range(per_device):
        y, x = pos[0, base + i], pos[1, base + i]
        hit = (i < count) & (y >= low) & (y < low + height)
        for c in range(CAP):
            this = hit & (seen == c)
            found[c] = jnp.where(this, i, found[c])
            ys[c] = jnp.where(this, y - low, ys[c])
            xs[c] = jnp.where(this, x, xs[c])
            lives[c] = jnp.where(this, 1, lives[c])
        seen = seen + hit.astype(jnp.int32)
    return found, ys, xs, lives


def pack_kernel(sizes, obj, pat, pos_in, cnt_in, ty_a, ty_b, tx_a, tx_b, held, rows, columns, pos, cnt, sems):
    slices, tile, margin = obj.shape[0], obj.shape[2], rows.shape[3]
    planes, tiles = slices * 2, obj.shape[3] // LANES
    row, col = lax.axis_index("ty"), lax.axis_index("tx")
    up_y, up_x = ups(row), ups(col)
    copies = [
        pltpu.make_async_copy(pos_in, pos, sems.at[0]),
        pltpu.make_async_copy(cnt_in, cnt, sems.at[1]),
        pltpu.make_async_copy(pat, held, sems.at[2]),
    ]
    for k in range(2):
        start = pl.multiple_of(up_y[k] * (tile - margin), margin)
        copies.append(pltpu.make_async_copy(obj.at[:, :, pl.ds(start, margin), :], rows.at[k], sems.at[3 + k]))
    for j in range(2):
        lane = pl.multiple_of(up_x[j] * (tile - LANES), LANES)
        copies.append(pltpu.make_async_copy(obj.at[:, :, :, pl.ds(lane, LANES)], columns.at[j], sems.at[5 + j]))
    for copy in copies:
        copy.start()
    for copy in copies[:3]:
        copy.wait()
    target = pick(row, sizes[2][0]) * tile
    found = slot_scan(pos, cnt, sizes, row, col, pat.shape[0], target, tile)[0]
    for c in range(CAP):
        for h in range(2):
            ty_a[planes * tiles + 2 * c + h] = held[found[c], h * margin : (h + 1) * margin, :]
    for k, out in enumerate((ty_a, ty_b)):
        copies[3 + k].wait()
        for p in range(planes):
            for t in range(tiles):
                block = rows[k, p // 2, p % 2, :, t * LANES : (t + 1) * LANES]
                out[p * tiles + t] = block.astype(BF16)
    for j, out in enumerate((tx_a, tx_b)):
        copies[5 + j].wait()
        for s in range(slices):
            re, im = columns[j, s, 0], columns[j, s, 1]
            packed = jnp.where(half_mask(tile, up_x[j]), re, pltpu.roll(im, LANES // 2, 1))
            out[s] = packed.astype(BF16)


def tile_kernel(sizes, obj, pat, pos, cnt, *refs):
    rounds = sizes[2]
    sources, ext, grad = refs[:3], refs[3], refs[4]
    routed, near_tables, sems = refs[5:-4], refs[-4:-1], refs[-1]
    slices, tile = obj.shape[0], obj.shape[2]
    tiles = obj.shape[3] // LANES
    margin = (ext.shape[2] - tile) // 2
    copies = []
    for p in range(slices * 2):
        for t in range(tiles):
            copies.append(
                pltpu.make_async_copy(
                    obj.at[p // 2, p % 2, :, t * LANES : (t + 1) * LANES],
                    ext.at[p, 1 + t, margin : margin + tile, :],
                    sems.at[p * tiles + t],
                )
            )
    for i, (a, b) in enumerate(zip(sources, near_tables)):
        copies.append(pltpu.make_async_copy(a, b, sems.at[slices * 2 * tiles + i]))
    for copy in copies:
        copy.start()
    row, col = lax.axis_index("ty"), lax.axis_index("tx")
    targets = [pick(row, partner) * tile for partner in rounds[1:]]
    found = [slot_scan(pos, cnt, sizes, row, col, pat.shape[0], t, tile)[0] for t in targets]
    for k, out in enumerate(routed):
        for c in range(CAP):
            out[c] = pat[found[k][c]]
    grad[...] = jnp.zeros(grad.shape, F32)
    for copy in copies:
        copy.wait()


def corner_kernel(slices, tiles, ty_a, ty_b, out_a, out_b):
    up_x = ups(lax.axis_index("tx"))
    for j, out in enumerate((out_a, out_b)):
        at = up_x[j] * (tiles - 1)
        for k, rows in enumerate((ty_a, ty_b)):
            for s in range(slices):
                re = rows[2 * s * tiles + at].astype(F32)
                im = rows[(2 * s + 1) * tiles + at].astype(F32)
                packed = jnp.where(half_mask(re.shape[0], up_x[j]), re, pltpu.roll(im, LANES // 2, 1))
                out[k * slices + s] = packed.astype(BF16)


def cmul(a, b):
    return a[0] * b[0] - a[1] * b[1], a[0] * b[1] + a[1] * b[0]


def cmul_conj(a, b):
    return a[0] * b[0] + a[1] * b[1], a[0] * b[1] - a[1] * b[0]


def transform(fields, right, left):
    extent = fields[0][0].shape[0]
    joined = jnp.concatenate([jnp.concatenate([re, im], 1) for re, im in fields], 0).astype(BF16)
    half = jnp.dot(joined, right, preferred_element_type=F32).astype(BF16)
    blocks = []
    for m in range(len(fields)):
        part = half[m * extent : (m + 1) * extent]
        blocks.append(jnp.concatenate([part[:, :extent], part[:, extent:]], 0))
    whole = jnp.dot(left, jnp.concatenate(blocks, 1), preferred_element_type=F32)
    return [
        (whole[:extent, m * extent : (m + 1) * extent], whole[extent:, m * extent : (m + 1) * extent])
        for m in range(len(fields))
    ]


def find_slots(sizes, pos, cnt, per_device, tile, row_of, col_of, live_of):
    rounds = sizes[2]
    row, col = lax.axis_index("ty"), lax.axis_index("tx")
    own = None
    for k in range(len(rounds) + 1):
        source = row if k == 0 else pick(row, rounds[k - 1])
        found, ys, xs, lives = slot_scan(pos, cnt, sizes, source, col, per_device, row * tile, tile)
        own = found if k == 0 else own
        for c in range(CAP):
            slot = k * CAP + c
            row_of[slot] = ys[c]
            col_of[slot] = jnp.where(lives[c] == 1, xs[c] - col * tile, 0)
            if live_of is not None:
                live_of[slot] = lives[c].astype(F32)
    return own


def places(row_of, col_of, slot, margin, lanes):
    x = col_of[slot] + margin
    off = x & (LANES - 1)
    return row_of[slot], lax.shift_right_logical(x, 7), off, lanes >= off


def window(ext, place, p):
    y, side, off, upper = place
    v0 = ext[p, side, pl.ds(y, LANES), :]
    v1 = ext[p, side + 1, pl.ds(y, LANES), :]
    return pltpu.roll(jnp.where(upper, v0, v1), (LANES - off) & (LANES - 1), 1)


def forward_kernel(sizes, per_device, pos, cnt, probe, first, second, kern, *refs):
    ty_in, tx_in, corner_in = refs[:2], refs[2:4], refs[4:6]
    ext, psi, waves, row_of, col_of = refs[7:]
    modes, extent = probe.shape[0], probe.shape[2]
    planes, margin, tiles = ext.shape[0], extent // 2, ext.shape[1] - 2
    slices, tile = planes // 2, ext.shape[2] - extent
    up_y, up_x = ups(lax.axis_index("ty")), ups(lax.axis_index("tx"))
    find_slots(sizes, pos, cnt, per_device, tile, row_of, col_of, None)
    for k in range(2):
        rows = pl.ds(pl.multiple_of(up_y[k] * (tile + margin), margin), margin)
        for p in range(planes):
            for t in range(tiles):
                ext[p, 1 + t, rows] = ty_in[k][p * tiles + t].astype(F32)
        for s in range(slices):
            for j in range(2):
                side = up_x[j] * (tiles + 1)
                strip = corner_in[j][k * slices + s].astype(F32)
                ext[2 * s, side, rows] = strip
                ext[2 * s + 1, side, rows] = pltpu.roll(strip, LANES // 2, 1)
    for s in range(slices):
        for j in range(2):
            side = up_x[j] * (tiles + 1)
            strip = tx_in[j][s].astype(F32)
            ext[2 * s, side, margin : margin + tile] = strip
            ext[2 * s + 1, side, margin : margin + tile] = pltpu.roll(strip, LANES // 2, 1)
    lanes = lane_ids(extent)

    def body(i, carry):
        slots = [i * BATCH + b for b in range(BATCH)]
        p_tab, q_tab = first[...], second[...]
        prop = (kern[0], kern[1])
        where = [places(row_of, col_of, slot, margin, lanes) for slot in slots]
        fields = [(probe[m, 0], probe[m, 1]) for m in range(modes)] * BATCH
        for s in range(slices):
            cells = [(window(ext, w, 2 * s), window(ext, w, 2 * s + 1)) for w in where]
            exits = [cmul(w, cells[n // modes]) for n, w in enumerate(fields)]
            far_field = transform(exits, p_tab, q_tab)
            if s + 1 < slices:
                fields = transform([cmul(prop, f) for f in far_field], q_tab, p_tab)
            kept = fields if s + 1 < slices else far_field
            for n, (re, im) in enumerate(kept):
                at = 2 * (n % modes)
                if s + 1 < slices:
                    waves[s, slots[n // modes], at] = re
                    waves[s, slots[n // modes], at + 1] = im
                else:
                    psi[slots[n // modes], at] = re
                    psi[slots[n // modes], at + 1] = im
        return carry

    lax.fori_loop(0, psi.shape[0] // BATCH, body, 0)


def backward_kernel(sizes, pat, pos, cnt, probe, first, second, kern, ext, psi, waves, *refs):
    _, n_tx, rounds = sizes
    k_n = len(rounds)
    pat_in, refs = refs[:k_n], refs[k_n + 1 :]
    grad, ty_out, keep, share = refs[0], refs[1:3], refs[3], refs[4]
    amp, acc, row_of, col_of, live_of = refs[5:]
    modes, extent = probe.shape[0], probe.shape[2]
    planes, margin, tiles = ext.shape[0], extent // 2, ext.shape[1] - 2
    slices, tile = planes // 2, ext.shape[2] - extent
    parts = planes * tiles
    row, col = lax.axis_index("ty"), lax.axis_index("tx")
    up_y, up_x = ups(row), ups(col)
    start_y = [pl.multiple_of(up_y[k] * (tile + margin), margin) for k in range(2)]
    own = find_slots(sizes, pos, cnt, pat.shape[0], tile, row_of, col_of, live_of)
    for c in range(CAP):
        amp[c] = pat[own[c]]
        for h in range(2):
            amp[CAP + c, h * margin : (h + 1) * margin] = pat_in[0][parts + 2 * c + h]
        for k in range(1, k_n):
            amp[(k + 1) * CAP + c] = pat_in[k][c]
    acc[...] = jnp.zeros(acc.shape, F32)
    lanes = lane_ids(extent)

    def scatter(place, p, value):
        y, side, off, upper = place
        moved = pltpu.roll(value, off, 1)
        grad[p, side, pl.ds(y, extent), :] += jnp.where(upper, moved, 0.0)
        grad[p, side + 1, pl.ds(y, extent), :] += jnp.where(upper, 0.0, moved)

    def body(i, carry):
        slots = [i * BATCH + b for b in range(BATCH)]
        p_tab, q_tab = first[...], second[...]
        prop = (kern[0], kern[1])
        where = [places(row_of, col_of, slot, margin, lanes) for slot in slots]
        residues = []
        for slot in slots:
            mine = [(psi[slot, 2 * m], psi[slot, 2 * m + 1]) for m in range(modes)]
            total = mine[0][0] * mine[0][0] + mine[0][1] * mine[0][1]
            for re, im in mine[1:]:
                total = total + (re * re + im * im)
            scale = amp[slot].astype(F32) * lax.rsqrt(jnp.maximum(total, 0.25))
            factor = (1.0 - scale) * live_of[slot]
            residues += [(re * factor, im * factor) for re, im in mine]
        back_waves = transform(residues, q_tab, p_tab)
        for s in reversed(range(slices)):
            for n, slot in enumerate(slots):
                for m in range(modes):
                    if s == 0:
                        wave = (probe[m, 0], probe[m, 1])
                    else:
                        wave = (waves[s - 1, slot, 2 * m], waves[s - 1, slot, 2 * m + 1])
                    re, im = cmul_conj(wave, back_waves[n * modes + m])
                    q_re, q_im = (re, im) if m == 0 else (q_re + re, q_im + im)
                scatter(where[n], 2 * s, q_re)
                scatter(where[n], 2 * s + 1, q_im)
            cells = [(window(ext, w, 2 * s), window(ext, w, 2 * s + 1)) for w in where]
            terms = [cmul_conj(cells[n // modes], g) for n, g in enumerate(back_waves)]
            if s > 0:
                inner = transform(terms, p_tab, q_tab)
                back_waves = transform([cmul_conj(prop, f) for f in inner], q_tab, p_tab)
        for m in range(modes):
            for c in range(2):
                value = terms[m][c]
                for n in range(1, BATCH):
                    value = value + terms[n * modes + m][c]
                acc[2 * m + c] += value
        return carry

    lax.fori_loop(0, psi.shape[0] // BATCH, body, 0)

    chunk = keep.shape[1]
    core = lax.rem(col, 2)
    for i in range(n_tx // 2):
        for out, parity in ((keep, core), (share, 1 - core)):
            at = (2 * i + parity) * chunk
            index = lax.div(at, extent)
            inside = pl.multiple_of(at - index * extent, chunk)
            out[i] = acc[index, pl.ds(inside, chunk), :]
    for k in range(2):
        for p in range(planes):
            for t in range(tiles):
                ty_out[k][p * tiles + t] = grad[p, 1 + t, pl.ds(start_y[k], margin)].astype(BF16)
        for j in range(2):
            side, mask = up_x[j] * (tiles + 1), half_mask(margin, 1 - up_x[j])
            for s in range(slices):
                re = grad[2 * s, side, pl.ds(start_y[k], margin)]
                im = grad[2 * s + 1, side, pl.ds(start_y[k], margin)]
                packed = jnp.where(mask, re, pltpu.roll(im, LANES // 2, 1))
                ty_out[k][parts + j * slices + s] = packed.astype(BF16)


def pair_kernel(keep, share, own, *outs):
    at = lax.shift_right_logical(lax.axis_index("tx"), 1)
    own[...] = keep[at] + share[at]
    for k, out in enumerate(outs, 1):
        other = jnp.bitwise_xor(at, k)
        out[...] = (keep[other] + share[other]).astype(BF16)


def join_kernel(*refs):
    parts, out = refs[:-1], refs[-1]
    at = lax.shift_right_logical(lax.axis_index("tx"), 1)
    for k, part in enumerate(parts):
        out[jnp.bitwise_xor(at, k)] = part[...]


def share_kernel(own, *refs):
    parts, out = refs[:-1], refs[-1]
    total = own[...]
    for part in parts:
        total = total + part[...].astype(F32)
    out[...] = total.astype(out.dtype)


def update_rate(probe):
    extent = probe.shape[2]
    power = jnp.sum(probe[...] * probe[...]) / (extent * extent)
    return jnp.full((1, 1), 1.0, F32) / (power + 1e-06)


def fold_kernel(tile, old, ty_a, ty_b, tx_a, tx_b, grad):
    planes, tiles = grad.shape[0], grad.shape[1] - 2
    slices, margin = planes // 2, (grad.shape[2] - tile) // 2
    up_y, up_x = ups(lax.axis_index("ty")), ups(lax.axis_index("tx"))
    for k, strips in enumerate((ty_a, ty_b)):
        rows = pl.ds(pl.multiple_of(margin + up_y[k] * (tile - margin), margin), margin)
        for p in range(planes):
            for t in range(tiles):
                grad[p, 1 + t, rows] += strips[p * tiles + t].astype(F32)
        for j in range(2):
            side, mask = up_x[j] * (tiles + 1), half_mask(margin, 1 - up_x[j])
            for s in range(slices):
                strip = strips[planes * tiles + j * slices + s].astype(F32)
                grad[2 * s, side, rows] += jnp.where(mask, strip, 0.0)
                grad[2 * s + 1, side, rows] += jnp.where(mask, pltpu.roll(strip, LANES // 2, 1), 0.0)
    inner = slice(margin, margin + tile)
    for j, out in enumerate((tx_a, tx_b)):
        side, mask = up_x[j] * (tiles + 1), half_mask(tile, 1 - up_x[j])
        for s in range(slices):
            re, im = grad[2 * s, side, inner], grad[2 * s + 1, side, inner]
            out[s] = jnp.where(mask, re, pltpu.roll(im, LANES // 2, 1)).astype(BF16)


def middle_kernel(obj, grad, probe, out, fresh, sems):
    tile, tiles = obj.shape[2], obj.shape[3] // LANES
    margin = (grad.shape[2] - tile) // 2
    rate = update_rate(probe)
    copies = []
    for p in range(obj.shape[0] * 2):
        s, c = p // 2, p % 2
        for t in range(1, tiles - 1):
            piece = obj[s, c, :, t * LANES : (t + 1) * LANES] - grad[p, 1 + t, margin : margin + tile] * rate
            fresh[s, c, :, (t - 1) * LANES : t * LANES] = piece
        copies.append(
            pltpu.make_async_copy(
                fresh.at[s, c], out.at[s, c, :, LANES : (tiles - 1) * LANES], sems.at[p]
            )
        )
        copies[-1].start()
    for copy in copies:
        copy.wait()


def edges_kernel(obj, grad, tx_a, tx_b, probe, old, out, fresh, sems):
    slices, tile, tiles = obj.shape[0], obj.shape[2], obj.shape[3] // LANES
    margin = (grad.shape[2] - tile) // 2
    up_x = ups(lax.axis_index("tx"))
    rate = update_rate(probe)
    copies = []
    for high in range(2):
        t, mask = high * (tiles - 1), half_mask(tile, high)
        span = slice(t * LANES, (t + 1) * LANES)
        for s in range(slices):
            strip = jnp.where(up_x[0] == high, tx_a[s].astype(F32), tx_b[s].astype(F32))
            for c in range(2):
                if c == 1:
                    strip = pltpu.roll(strip, LANES // 2, 1)
                total = grad[2 * s + c, 1 + t, margin : margin + tile] + jnp.where(mask, strip, 0.0)
                fresh[high, s, c] = obj[s, c, :, span] - total * rate
            copies.append(
                pltpu.make_async_copy(fresh.at[high, s], out.at[s, :, :, span], sems.at[high * slices + s])
            )
            copies[-1].start()
    for copy in copies:
        copy.wait()


def probe_kernel(probe, joined, other, out, held):
    modes, extent, chunk = probe.shape[0], probe.shape[2], joined.shape[1]
    core = lax.rem(lax.axis_index("tx"), 2)
    for i in range(joined.shape[0]):
        for part, parity in ((joined, core), (other, 1 - core)):
            at = pl.multiple_of((2 * i + parity) * chunk, chunk)
            held[pl.ds(at, chunk), :] = part[i].astype(F32)
    summed = held[...]
    mean = jnp.sum(summed * summed) / summed.size
    step = jnp.full((1, 1), 0.5, F32) * lax.rsqrt(jnp.full((1, 1), 1.0, F32) * (mean + 1e-06))
    for m in range(modes):
        for c in range(2):
            at = (2 * m + c) * extent
            out[m, c] = probe[m, c] - held[at : at + extent] * step


def sum_kernel(sizes, own, *refs):
    rounds = sizes[2]
    parts, out, held = refs[: len(rounds)], refs[len(rounds)], refs[len(rounds) + 1]
    row = lax.axis_index("ty")
    held[row] = own[...].astype(F32)
    for k, partner in enumerate(rounds):
        held[pick(row, partner)] = parts[k][...].astype(F32)
    total = held[0]
    for i in range(1, held.shape[0]):
        total = total + held[i]
    out[...] = total.astype(out.dtype)


BATCH = 4
VMEM_BYTES = 10 * 1024 * 1024
VMEM = pl.BlockSpec(memory_space=pltpu.VMEM)
SMEM = pl.BlockSpec(memory_space=pltpu.SMEM)
ANY = pl.BlockSpec(memory_space=pl.ANY)


def call(kernel, operands, specs, outs, scratch=(), aliases=None, out_specs=None):
    single = not isinstance(outs, (list, tuple))
    return pl.pallas_call(
        kernel,
        out_shape=outs,
        in_specs=specs,
        out_specs=out_specs or (VMEM if single else [VMEM] * len(outs)),
        scratch_shapes=list(scratch),
        input_output_aliases=aliases or {},
        compiler_params=pltpu.CompilerParams(vmem_limit_bytes=VMEM_BYTES),
    )(*operands)


def near(value):
    return pltpu.with_memory_space_constraint(value, pltpu.VMEM)


def far(value):
    return pltpu.with_memory_space_constraint(value, pltpu.HBM)


def send(value, axis, pairs):
    return near(lax.ppermute(value, axis, pairs))


def step(object_slices, probe_modes, patterns, positions, counts):
    slices, _, tile, _ = object_slices.shape
    modes, _, extent, _ = probe_modes.shape
    margin, tiles = extent // 2, tile // LANES
    n_ty, n_tx = lax.axis_size("ty"), lax.axis_size("tx")
    rounds = pairings(n_ty)
    sizes = (n_ty, n_tx, rounds)
    parts = slices * 2 * tiles
    k_n = len(rounds)
    places = positions.T
    planes = slices * 2
    block = (margin, LANES)
    strips = [pltpu.VMEM((slices, tile, LANES), BF16)] * 2
    strips = [pltpu.VMEM((slices, tile, LANES), BF16)] * 2
    rows_out = [pltpu.VMEM((parts + 2 * slices,) + block, BF16)] * 2
    ty_a, ty_b, tx_a, tx_b, near_patterns = call(
        lambda *r: pack_kernel(sizes, *r),
        (far(object_slices), far(patterns), far(places), far(counts)),
        [ANY] * 4,
        [pltpu.VMEM((parts + extra,) + block, BF16) for extra in (2 * CAP, 0)]
        + strips
        + [pltpu.VMEM(patterns.shape, BF16)],
        [
            pltpu.VMEM((2, slices, 2, margin, tile), F32),
            pltpu.VMEM((2, slices, 2, tile, LANES), F32),
            pltpu.SMEM(places.shape, jnp.int32),
            pltpu.SMEM(counts.shape, jnp.int32),
            pltpu.SemaphoreType.DMA((7,)),
        ],
    )
    near_object, near_patterns = near(object_slices), near(near_patterns)

    def pair_rows(value, k):
        return send(value, "ty", [(i, rounds[k][i]) for i in range(n_ty)])

    def swap(value, axis, side):
        return send(value, axis, neighbour_pairs(side, lax.axis_size(axis)))

    def cross(value, k):
        return send(value, "tx", [(i, i ^ k) for i in range(n_tx)])

    ext_shape = (planes, tiles + 2, tile + extent, LANES)
    ty_in = [swap(ty_a, "ty", 0), swap(ty_b, "ty", 1)]
    tx_in = [swap(tx_a, "tx", 0), swap(tx_b, "tx", 1)]
    tables = make_tables(extent)
    ext, grad, *routed, first, second, kern = call(
        lambda *r: tile_kernel(sizes, *r),
        (far(object_slices), near_patterns, far(places), far(counts))
        + tuple(far(c) for c in tables),
        [ANY, VMEM, SMEM, SMEM] + [ANY] * 3,
        [pltpu.VMEM(ext_shape, F32)] * 2
        + [pltpu.VMEM((CAP, extent, extent), BF16)] * (k_n - 1)
        + [pltpu.VMEM(c.shape, c.dtype) for c in tables],
        [pltpu.SemaphoreType.DMA((parts + 3,))],
    )
    constants = tuple(near(c) for c in (first, second, kern))
    corners = call(
        lambda *r: corner_kernel(slices, tiles, *r),
        tuple(ty_in),
        [VMEM] * 2,
        [pltpu.VMEM((2 * slices,) + block, BF16)] * 2,
    )
    corner_in = [swap(corners[j], "tx", j) for j in range(2)]
    pat_in = [ty_in[0]] + [pair_rows(routed[k - 1], k) for k in range(1, k_n)]

    slots = (k_n + 1) * CAP
    chunk = modes * 2 * extent // n_tx
    field = (slots, 2 * modes, extent, extent)
    places_near = [pltpu.SMEM((slots,), jnp.int32)] * 2
    ext, psi, waves = call(
        lambda *r: forward_kernel(sizes, patterns.shape[0], *r),
        (places, counts, near(probe_modes))
        + constants
        + tuple(ty_in + tx_in + corner_in)
        + (near(ext),),
        [SMEM, SMEM] + [VMEM] * 11,
        [pltpu.VMEM(ext_shape, F32), pltpu.VMEM(field, F32), pltpu.VMEM((slices - 1,) + field, F32)],
        places_near,
        {12: 0},
    )
    results = call(
        lambda *r: backward_kernel(sizes, *r),
        (near_patterns, places, counts, near(probe_modes))
        + constants
        + (near(ext), near(psi), near(waves), *pat_in, near(grad)),
        [VMEM, SMEM, SMEM] + [VMEM] * (7 + k_n + 1),
        [pltpu.VMEM(ext_shape, F32)]
        + rows_out
        + [pltpu.VMEM((n_tx // 2, chunk, LANES), F32)] * 2,
        [pltpu.VMEM((slots, extent, extent), BF16), pltpu.VMEM((2 * modes, extent, extent), F32)]
        + places_near
        + [pltpu.SMEM((slots,), F32)],
        {10 + k_n: 0},
    )
    grad, ty_a, ty_b, keep, share = results
    ty_back = [swap(ty_a, "ty", 0), swap(ty_b, "ty", 1)]
    mine, *shares = call(
        pair_kernel,
        (near(keep), cross(share, 1)),
        [VMEM] * 2,
        [pltpu.VMEM((chunk, LANES), F32)] + [pltpu.VMEM((chunk, LANES), BF16)] * (n_tx // 2 - 1),
    )
    others = tuple(cross(shares[k - 1], 2 * k) for k in range(1, n_tx // 2))
    mine = call(
        share_kernel, (near(mine),) + others, [VMEM] * (n_tx // 2), pltpu.VMEM((chunk, LANES), BF16)
    )
    rows_in = tuple(pair_rows(mine, k) for k in range(k_n))
    tx_a, tx_b, grad = call(
        lambda *r: fold_kernel(tile, *r),
        (near(grad), *ty_back),
        [VMEM] * 3,
        strips + [pltpu.VMEM(ext_shape, F32)],
        (),
        {0: 2},
    )
    tx_back = [swap(tx_a, "tx", 0), swap(tx_b, "tx", 1)]
    full = call(
        lambda *r: sum_kernel(sizes, *r),
        (near(mine),) + rows_in,
        [VMEM] * (k_n + 1),
        pltpu.VMEM((chunk, LANES), BF16),
        [pltpu.VMEM((n_ty, chunk, LANES), F32)],
    )
    gathered = tuple(cross(full, 2 * k) for k in range(1, n_tx // 2))
    joined = call(
        join_kernel,
        (near(full),) + gathered,
        [VMEM] * (n_tx // 2),
        pltpu.VMEM((n_tx // 2, chunk, LANES), BF16),
    )
    other = cross(joined, 1)
    partial = call(
        middle_kernel,
        (near_object, near(grad), near(probe_modes)),
        [VMEM] * 3,
        pltpu.HBM(object_slices.shape, F32),
        [pltpu.VMEM((slices, 2, tile, tile - 2 * LANES), F32), pltpu.SemaphoreType.DMA((planes,))],
        None,
        ANY,
    )
    new_object = call(
        edges_kernel,
        (near_object, near(grad), *tx_back, near(probe_modes), far(partial)),
        [VMEM] * 5 + [ANY],
        pltpu.HBM(object_slices.shape, F32),
        [
            pltpu.VMEM((2, slices, 2, tile, LANES), F32),
            pltpu.SemaphoreType.DMA((2 * slices,)),
        ],
        {5: 0},
        ANY,
    )
    new_probe = call(
        probe_kernel,
        (near(probe_modes), near(joined), other),
        [VMEM] * 3,
        jax.ShapeDtypeStruct(probe_modes.shape, F32),
        [pltpu.VMEM((modes * 2 * extent, LANES), F32)],
    )
    return (new_object, new_probe)


def solution(mesh):
    return jax.shard_map(
        step,
        mesh=mesh,
        in_specs=(P(None, None, "ty", "tx"), P(), P(("ty", "tx"), None, None), P(), P()),
        out_specs=(P(None, None, "ty", "tx"), P()),
        check_vma=False,
    )
```

```python
import math

import numpy as np
import jax
import jax.numpy as jnp
from jax import lax
from jax.experimental import pallas as pl
from jax.experimental.pallas import tpu as pltpu
from jax.sharding import PartitionSpec as P


CAP = 2
PROPAGATION = 0.37
LANES = 128
BF16 = jnp.bfloat16
F32 = jnp.float32


def make_tables(extent):
    indices = np.arange(extent, dtype=np.int32)
    product = indices[:, None] * indices[None, :] % extent
    angles = np.float32(2.0 * math.pi / extent) * product.astype(np.float32)
    norm_scale = np.float32(1.0 / math.sqrt(extent))
    real_table = jnp.asarray(np.cos(angles) * norm_scale, F32).astype(BF16)
    imag_table = jnp.asarray(-np.sin(angles) * norm_scale, F32).astype(BF16)
    first = jnp.concatenate(
        [
            jnp.concatenate([real_table, imag_table], 1),
            jnp.concatenate([-imag_table, real_table], 1),
        ],
        0,
    )
    second = jnp.concatenate(
        [
            jnp.concatenate([real_table, -imag_table], 1),
            jnp.concatenate([imag_table, real_table], 1),
        ],
        0,
    )
    frequency = np.where(indices < extent // 2, indices, indices - extent).astype(np.float32)
    phases = np.float32(-math.pi * PROPAGATION / extent) * (
        frequency[:, None] ** 2 + frequency[None, :] ** 2
    )
    kernel = jnp.asarray(np.stack([np.cos(phases), np.sin(phases)]), F32)
    return first, second, kernel


def pairings(n):
    if n == 2:
        return [[1, 0]]
    assert n % 2 == 0 and all((n - 1) % d for d in range(2, n - 1))
    odd = n - 1
    rounds = []
    for k in range(odd):
        partner = [0] * n
        partner[odd], partner[k] = k, odd
        for i in range(1, n // 2):
            a, b = (k + i) % odd, (k - i) % odd
            partner[a], partner[b] = b, a
        rounds.append(partner)
    order = [odd]
    while len(order) < n:
        order.append(rounds[(len(order) - 1) % 2][order[-1]])
    label = {v: i for i, v in enumerate(order)}
    return [[label[r[order[i]]] for i in range(n)] for r in rounds]


def neighbour(side, i):
    return 1 if (i + side) % 2 == 0 else -1


def neighbour_pairs(side, n):
    steps = [(i, i + neighbour(side, i)) for i in range(n)]
    return [(i, j) for i, j in steps if 0 <= j < n]


def pick(index, values):
    chosen = jnp.int32(values[0])
    for i in range(1, len(values)):
        chosen = jnp.where(index == i, jnp.int32(values[i]), chosen)
    return chosen


def lane_ids(rows):
    return lax.broadcasted_iota(jnp.int32, (rows, LANES), 1)


def half_mask(rows, upper):
    return (lane_ids(rows) >= LANES // 2).astype(jnp.int32) == upper


def ups(index):
    even = 1 - lax.rem(index, 2)
    return [even, 1 - even]


def slot_scan(pos, cnt, sizes, source, col, per_device, low, height):
    n_tx = sizes[1]
    base = (source * n_tx + col) * per_device
    count = cnt[source * n_tx + col]
    zero = jnp.int32(0)
    found, ys, xs, lives = [zero] * CAP, [zero] * CAP, [zero] * CAP, [zero] * CAP
    seen = zero
    for i in range(per_device):
        y, x = pos[0, base + i], pos[1, base + i]
        hit = (i < count) & (y >= low) & (y < low + height)
        for c in range(CAP):
            this = hit & (seen == c)
            found[c] = jnp.where(this, i, found[c])
            ys[c] = jnp.where(this, y - low, ys[c])
            xs[c] = jnp.where(this, x, xs[c])
            lives[c] = jnp.where(this, 1, lives[c])
        seen = seen + hit.astype(jnp.int32)
    return found, ys, xs, lives


def pack_kernel(sizes, obj, pat, pos_in, cnt_in, ty_a, ty_b, tx_a, tx_b, held, ext, grad, *refs):
    routed, (rows, pos, cnt, sems) = refs[:-4], refs[-4:]
    slices, tile, margin = obj.shape[0], obj.shape[2], rows.shape[3]
    planes, tiles = slices * 2, obj.shape[3] // LANES
    row, col = lax.axis_index("ty"), lax.axis_index("tx")
    up_y, up_x = ups(row), ups(col)
    copies = [
        pltpu.make_async_copy(pos_in, pos, sems.at[0]),
        pltpu.make_async_copy(cnt_in, cnt, sems.at[1]),
        pltpu.make_async_copy(pat, held, sems.at[2]),
    ]
    for k in range(2):
        start = pl.multiple_of(up_y[k] * (tile - margin), margin)
        copies.append(pltpu.make_async_copy(obj.at[:, :, pl.ds(start, margin), :], rows.at[k], sems.at[3 + k]))
    outer = sorted({0, tiles - 1})
    inner = slice(margin, margin + tile)
    for p in range(planes):
        for i, t in enumerate(outer):
            lanes = slice(t * LANES, (t + 1) * LANES)
            copies.append(
                pltpu.make_async_copy(
                    obj.at[p // 2, p % 2, :, lanes], ext.at[p, 1 + t, inner, :], sems.at[5 + 2 * p + i]
                )
            )
    for copy in copies:
        copy.start()
    for copy in copies[:3]:
        copy.wait()
    target = pick(row, sizes[2][0]) * tile
    found = slot_scan(pos, cnt, sizes, row, col, pat.shape[0], target, tile)[0]
    for c in range(CAP):
        for h in range(2):
            ty_a[planes * tiles + 2 * c + h] = held[found[c], h * margin : (h + 1) * margin, :]
    for k, out in enumerate((ty_a, ty_b)):
        copies[3 + k].wait()
        for p in range(planes):
            for t in range(tiles):
                block = rows[k, p // 2, p % 2, :, t * LANES : (t + 1) * LANES]
                out[p * tiles + t] = block.astype(BF16)
    grad[...] = jnp.zeros(grad.shape, F32)
    for k, out in enumerate(routed, 1):
        target = pick(row, sizes[2][k]) * tile
        found = slot_scan(pos, cnt, sizes, row, col, pat.shape[0], target, tile)[0]
        for c in range(CAP):
            out[c] = held[found[c]]
    for copy in copies[5:]:
        copy.wait()
    for j, out in enumerate((tx_a, tx_b)):
        side = 1 + up_x[j] * (tiles - 1)
        for s in range(slices):
            re, im = ext[2 * s, side, inner], ext[2 * s + 1, side, inner]
            packed = jnp.where(half_mask(tile, up_x[j]), re, pltpu.roll(im, LANES // 2, 1))
            out[s] = packed.astype(BF16)


def tile_kernel(obj, *refs):
    sources, ext, near_tables, sems = refs[:3], refs[4], refs[5:-1], refs[-1]
    slices, tile = obj.shape[0], obj.shape[2]
    tiles = obj.shape[3] // LANES
    margin = (ext.shape[2] - tile) // 2
    copies = []
    for p in range(slices * 2):
        for t in range(1, tiles - 1):
            copies.append(
                pltpu.make_async_copy(
                    obj.at[p // 2, p % 2, :, t * LANES : (t + 1) * LANES],
                    ext.at[p, 1 + t, margin : margin + tile, :],
                    sems.at[p * tiles + t],
                )
            )
    for i, (a, b) in enumerate(zip(sources, near_tables)):
        copies.append(pltpu.make_async_copy(a, b, sems.at[slices * 2 * tiles + i]))
    for copy in copies:
        copy.start()
    for copy in copies:
        copy.wait()


def corner_kernel(slices, tiles, ty_a, ty_b, out_a, out_b):
    up_x = ups(lax.axis_index("tx"))
    for j, out in enumerate((out_a, out_b)):
        at = up_x[j] * (tiles - 1)
        for k, rows in enumerate((ty_a, ty_b)):
            for s in range(slices):
                re = rows[2 * s * tiles + at].astype(F32)
                im = rows[(2 * s + 1) * tiles + at].astype(F32)
                packed = jnp.where(half_mask(re.shape[0], up_x[j]), re, pltpu.roll(im, LANES // 2, 1))
                out[k * slices + s] = packed.astype(BF16)


def cmul(a, b):
    return a[0] * b[0] - a[1] * b[1], a[0] * b[1] + a[1] * b[0]


def cmul_conj(a, b):
    return a[0] * b[0] + a[1] * b[1], a[0] * b[1] - a[1] * b[0]


def transform(fields, right, left):
    extent = fields[0][0].shape[0]
    joined = jnp.concatenate([jnp.concatenate([re, im], 1) for re, im in fields], 0).astype(BF16)
    half = jnp.dot(joined, right, preferred_element_type=F32).astype(BF16)
    blocks = []
    for m in range(len(fields)):
        part = half[m * extent : (m + 1) * extent]
        blocks.append(jnp.concatenate([part[:, :extent], part[:, extent:]], 0))
    whole = jnp.dot(left, jnp.concatenate(blocks, 1), preferred_element_type=F32)
    return [
        (whole[:extent, m * extent : (m + 1) * extent], whole[extent:, m * extent : (m + 1) * extent])
        for m in range(len(fields))
    ]


def find_slots(sizes, pos, cnt, per_device, tile, row_of, col_of, live_of):
    rounds = sizes[2]
    row, col = lax.axis_index("ty"), lax.axis_index("tx")
    own = None
    for k in range(len(rounds) + 1):
        source = row if k == 0 else pick(row, rounds[k - 1])
        found, ys, xs, lives = slot_scan(pos, cnt, sizes, source, col, per_device, row * tile, tile)
        own = found if k == 0 else own
        for c in range(CAP):
            slot = k * CAP + c
            row_of[slot] = ys[c]
            col_of[slot] = jnp.where(lives[c] == 1, xs[c] - col * tile, 0)
            if live_of is not None:
                live_of[slot] = lives[c].astype(F32)
    return own


def places(row_of, col_of, slot, margin, lanes):
    x = col_of[slot] + margin
    off = x & (LANES - 1)
    return row_of[slot], lax.shift_right_logical(x, 7), off, lanes >= off


def window(ext, place, p):
    y, side, off, upper = place
    v0 = ext[p, side, pl.ds(y, LANES), :]
    v1 = ext[p, side + 1, pl.ds(y, LANES), :]
    return pltpu.roll(jnp.where(upper, v0, v1), (LANES - off) & (LANES - 1), 1)


def forward_kernel(sizes, per_device, pos, cnt, probe, first, second, kern, *refs):
    ty_in, tx_in, corner_in = refs[:2], refs[2:4], refs[4:6]
    ext, psi, waves, row_of, col_of = refs[7:]
    modes, extent = probe.shape[0], probe.shape[2]
    planes, margin, tiles = ext.shape[0], extent // 2, ext.shape[1] - 2
    slices, tile = planes // 2, ext.shape[2] - extent
    up_y, up_x = ups(lax.axis_index("ty")), ups(lax.axis_index("tx"))
    find_slots(sizes, pos, cnt, per_device, tile, row_of, col_of, None)
    for k in range(2):
        rows = pl.ds(pl.multiple_of(up_y[k] * (tile + margin), margin), margin)
        for p in range(planes):
            for t in range(tiles):
                ext[p, 1 + t, rows] = ty_in[k][p * tiles + t].astype(F32)
        for s in range(slices):
            for j in range(2):
                side = up_x[j] * (tiles + 1)
                strip = corner_in[j][k * slices + s].astype(F32)
                ext[2 * s, side, rows] = strip
                ext[2 * s + 1, side, rows] = pltpu.roll(strip, LANES // 2, 1)
    for s in range(slices):
        for j in range(2):
            side = up_x[j] * (tiles + 1)
            strip = tx_in[j][s].astype(F32)
            ext[2 * s, side, margin : margin + tile] = strip
            ext[2 * s + 1, side, margin : margin + tile] = pltpu.roll(strip, LANES // 2, 1)
    lanes = lane_ids(extent)

    def body(i, carry):
        slots = [i * BATCH + b for b in range(BATCH)]
        p_tab, q_tab = first[...], second[...]
        prop = (kern[0], kern[1])
        where = [places(row_of, col_of, slot, margin, lanes) for slot in slots]
        fields = [(probe[m, 0], probe[m, 1]) for m in range(modes)] * BATCH
        for s in range(slices):
            cells = [(window(ext, w, 2 * s), window(ext, w, 2 * s + 1)) for w in where]
            exits = [cmul(w, cells[n // modes]) for n, w in enumerate(fields)]
            far_field = transform(exits, p_tab, q_tab)
            if s + 1 < slices:
                fields = transform([cmul(prop, f) for f in far_field], q_tab, p_tab)
            kept = fields if s + 1 < slices else far_field
            for n, (re, im) in enumerate(kept):
                at = 2 * (n % modes)
                if s + 1 < slices:
                    waves[s, slots[n // modes], at] = re
                    waves[s, slots[n // modes], at + 1] = im
                else:
                    psi[slots[n // modes], at] = re
                    psi[slots[n // modes], at + 1] = im
        return carry

    lax.fori_loop(0, psi.shape[0] // BATCH, body, 0)


def backward_kernel(sizes, pat, pos, cnt, probe, first, second, kern, ext, psi, waves, *refs):
    _, n_tx, rounds = sizes
    k_n = len(rounds)
    pat_in, refs = refs[:k_n], refs[k_n + 1 :]
    grad, ty_out, keep, share = refs[0], refs[1:3], refs[3], refs[4]
    amp, acc, row_of, col_of, live_of = refs[5:]
    modes, extent = probe.shape[0], probe.shape[2]
    planes, margin, tiles = ext.shape[0], extent // 2, ext.shape[1] - 2
    slices, tile = planes // 2, ext.shape[2] - extent
    parts = planes * tiles
    row, col = lax.axis_index("ty"), lax.axis_index("tx")
    up_y, up_x = ups(row), ups(col)
    start_y = [pl.multiple_of(up_y[k] * (tile + margin), margin) for k in range(2)]
    own = find_slots(sizes, pos, cnt, pat.shape[0], tile, row_of, col_of, live_of)
    for c in range(CAP):
        amp[c] = pat[own[c]]
        for h in range(2):
            amp[CAP + c, h * margin : (h + 1) * margin] = pat_in[0][parts + 2 * c + h]
        for k in range(1, k_n):
            amp[(k + 1) * CAP + c] = pat_in[k][c]
    acc[...] = jnp.zeros(acc.shape, F32)
    lanes = lane_ids(extent)

    def scatter(place, p, value):
        y, side, off, upper = place
        moved = pltpu.roll(value, off, 1)
        grad[p, side, pl.ds(y, extent), :] += jnp.where(upper, moved, 0.0)
        grad[p, side + 1, pl.ds(y, extent), :] += jnp.where(upper, 0.0, moved)

    def body(i, carry):
        slots = [i * BATCH + b for b in range(BATCH)]
        p_tab, q_tab = first[...], second[...]
        prop = (kern[0], kern[1])
        where = [places(row_of, col_of, slot, margin, lanes) for slot in slots]
        residues = []
        for slot in slots:
            mine = [(psi[slot, 2 * m], psi[slot, 2 * m + 1]) for m in range(modes)]
            total = mine[0][0] * mine[0][0] + mine[0][1] * mine[0][1]
            for re, im in mine[1:]:
                total = total + (re * re + im * im)
            scale = amp[slot].astype(F32) * lax.rsqrt(jnp.maximum(total, 0.25))
            factor = (1.0 - scale) * live_of[slot]
            residues += [(re * factor, im * factor) for re, im in mine]
        back_waves = transform(residues, q_tab, p_tab)
        for s in reversed(range(slices)):
            for n, slot in enumerate(slots):
                for m in range(modes):
                    if s == 0:
                        wave = (probe[m, 0], probe[m, 1])
                    else:
                        wave = (waves[s - 1, slot, 2 * m], waves[s - 1, slot, 2 * m + 1])
                    re, im = cmul_conj(wave, back_waves[n * modes + m])
                    q_re, q_im = (re, im) if m == 0 else (q_re + re, q_im + im)
                scatter(where[n], 2 * s, q_re)
                scatter(where[n], 2 * s + 1, q_im)
            cells = [(window(ext, w, 2 * s), window(ext, w, 2 * s + 1)) for w in where]
            terms = [cmul_conj(cells[n // modes], g) for n, g in enumerate(back_waves)]
            if s > 0:
                inner = transform(terms, p_tab, q_tab)
                back_waves = transform([cmul_conj(prop, f) for f in inner], q_tab, p_tab)
        for m in range(modes):
            for c in range(2):
                value = terms[m][c]
                for n in range(1, BATCH):
                    value = value + terms[n * modes + m][c]
                acc[2 * m + c] += value
        return carry

    lax.fori_loop(0, psi.shape[0] // BATCH, body, 0)

    chunk = keep.shape[1]
    core = lax.rem(col, 2)
    for i in range(n_tx // 2):
        for out, parity in ((keep, core), (share, 1 - core)):
            at = (2 * i + parity) * chunk
            index = lax.div(at, extent)
            inside = pl.multiple_of(at - index * extent, chunk)
            out[i] = acc[index, pl.ds(inside, chunk), :]
    for k in range(2):
        for p in range(planes):
            for t in range(tiles):
                ty_out[k][p * tiles + t] = grad[p, 1 + t, pl.ds(start_y[k], margin)].astype(BF16)
        for j in range(2):
            side, mask = up_x[j] * (tiles + 1), half_mask(margin, 1 - up_x[j])
            for s in range(slices):
                re = grad[2 * s, side, pl.ds(start_y[k], margin)]
                im = grad[2 * s + 1, side, pl.ds(start_y[k], margin)]
                packed = jnp.where(mask, re, pltpu.roll(im, LANES // 2, 1))
                ty_out[k][parts + j * slices + s] = packed.astype(BF16)


def pair_kernel(keep, share, own, *outs):
    at = lax.shift_right_logical(lax.axis_index("tx"), 1)
    own[...] = keep[at] + share[at]
    for k, out in enumerate(outs, 1):
        other = jnp.bitwise_xor(at, k)
        out[...] = (keep[other] + share[other]).astype(BF16)


def join_kernel(*refs):
    parts, out = refs[:-1], refs[-1]
    at = lax.shift_right_logical(lax.axis_index("tx"), 1)
    for k, part in enumerate(parts):
        out[jnp.bitwise_xor(at, k)] = part[...]


def share_kernel(own, *refs):
    parts, out = refs[:-1], refs[-1]
    total = own[...]
    for part in parts:
        total = total + part[...].astype(F32)
    out[...] = total.astype(out.dtype)


def update_rate(probe):
    extent = probe.shape[2]
    power = jnp.sum(probe[...] * probe[...]) / (extent * extent)
    return jnp.full((1, 1), 1.0, F32) / (power + 1e-06)


def fold_kernel(tile, old, ty_a, ty_b, tx_a, tx_b, grad):
    planes, tiles = grad.shape[0], grad.shape[1] - 2
    slices, margin = planes // 2, (grad.shape[2] - tile) // 2
    up_y, up_x = ups(lax.axis_index("ty")), ups(lax.axis_index("tx"))
    for k, strips in enumerate((ty_a, ty_b)):
        rows = pl.ds(pl.multiple_of(margin + up_y[k] * (tile - margin), margin), margin)
        for p in range(planes):
            for t in range(tiles):
                grad[p, 1 + t, rows] += strips[p * tiles + t].astype(F32)
        for j in range(2):
            side, mask = up_x[j] * (tiles + 1), half_mask(margin, 1 - up_x[j])
            for s in range(slices):
                strip = strips[planes * tiles + j * slices + s].astype(F32)
                grad[2 * s, side, rows] += jnp.where(mask, strip, 0.0)
                grad[2 * s + 1, side, rows] += jnp.where(mask, pltpu.roll(strip, LANES // 2, 1), 0.0)
    inner = slice(margin, margin + tile)
    for j, out in enumerate((tx_a, tx_b)):
        side, mask = up_x[j] * (tiles + 1), half_mask(tile, 1 - up_x[j])
        for s in range(slices):
            re, im = grad[2 * s, side, inner], grad[2 * s + 1, side, inner]
            out[s] = jnp.where(mask, re, pltpu.roll(im, LANES // 2, 1)).astype(BF16)


def middle_kernel(obj, grad, probe, out, fresh, sems):
    tile, tiles = obj.shape[2], obj.shape[3] // LANES
    margin = (grad.shape[2] - tile) // 2
    rate = update_rate(probe)
    copies = []
    for p in range(obj.shape[0] * 2):
        s, c = p // 2, p % 2
        for t in range(1, tiles - 1):
            piece = obj[s, c, :, t * LANES : (t + 1) * LANES] - grad[p, 1 + t, margin : margin + tile] * rate
            fresh[s, c, :, (t - 1) * LANES : t * LANES] = piece
        copies.append(
            pltpu.make_async_copy(
                fresh.at[s, c], out.at[s, c, :, LANES : (tiles - 1) * LANES], sems.at[p]
            )
        )
        copies[-1].start()
    for copy in copies:
        copy.wait()


def edges_kernel(obj, grad, tx_a, tx_b, probe, old, out, fresh, sems):
    slices, tile, tiles = obj.shape[0], obj.shape[2], obj.shape[3] // LANES
    margin = (grad.shape[2] - tile) // 2
    up_x = ups(lax.axis_index("tx"))
    rate = update_rate(probe)
    copies = []
    for high in range(2):
        t, mask = high * (tiles - 1), half_mask(tile, high)
        span = slice(t * LANES, (t + 1) * LANES)
        for s in range(slices):
            strip = jnp.where(up_x[0] == high, tx_a[s].astype(F32), tx_b[s].astype(F32))
            for c in range(2):
                if c == 1:
                    strip = pltpu.roll(strip, LANES // 2, 1)
                total = grad[2 * s + c, 1 + t, margin : margin + tile] + jnp.where(mask, strip, 0.0)
                fresh[high, s, c] = obj[s, c, :, span] - total * rate
            copies.append(
                pltpu.make_async_copy(fresh.at[high, s], out.at[s, :, :, span], sems.at[high * slices + s])
            )
            copies[-1].start()
    for copy in copies:
        copy.wait()


def probe_kernel(probe, joined, other, out, held):
    modes, extent, chunk = probe.shape[0], probe.shape[2], joined.shape[1]
    core = lax.rem(lax.axis_index("tx"), 2)
    for i in range(joined.shape[0]):
        for part, parity in ((joined, core), (other, 1 - core)):
            at = pl.multiple_of((2 * i + parity) * chunk, chunk)
            held[pl.ds(at, chunk), :] = part[i].astype(F32)
    summed = held[...]
    mean = jnp.sum(summed * summed) / summed.size
    step = jnp.full((1, 1), 0.5, F32) * lax.rsqrt(jnp.full((1, 1), 1.0, F32) * (mean + 1e-06))
    for m in range(modes):
        for c in range(2):
            at = (2 * m + c) * extent
            out[m, c] = probe[m, c] - held[at : at + extent] * step


def sum_kernel(sizes, own, *refs):
    rounds = sizes[2]
    parts, out, held = refs[: len(rounds)], refs[len(rounds)], refs[len(rounds) + 1]
    row = lax.axis_index("ty")
    held[row] = own[...].astype(F32)
    for k, partner in enumerate(rounds):
        held[pick(row, partner)] = parts[k][...].astype(F32)
    total = held[0]
    for i in range(1, held.shape[0]):
        total = total + held[i]
    out[...] = total.astype(out.dtype)


BATCH = 4
VMEM_BYTES = 10 * 1024 * 1024
VMEM = pl.BlockSpec(memory_space=pltpu.VMEM)
SMEM = pl.BlockSpec(memory_space=pltpu.SMEM)
ANY = pl.BlockSpec(memory_space=pl.ANY)


def call(kernel, operands, specs, outs, scratch=(), aliases=None, out_specs=None):
    single = not isinstance(outs, (list, tuple))
    return pl.pallas_call(
        kernel,
        out_shape=outs,
        in_specs=specs,
        out_specs=out_specs or (VMEM if single else [VMEM] * len(outs)),
        scratch_shapes=list(scratch),
        input_output_aliases=aliases or {},
        compiler_params=pltpu.CompilerParams(vmem_limit_bytes=VMEM_BYTES),
    )(*operands)


def near(value):
    return pltpu.with_memory_space_constraint(value, pltpu.VMEM)


def far(value):
    return pltpu.with_memory_space_constraint(value, pltpu.HBM)


def send(value, axis, pairs):
    return near(lax.ppermute(value, axis, pairs))


def step(object_slices, probe_modes, patterns, positions, counts):
    slices, _, tile, _ = object_slices.shape
    modes, _, extent, _ = probe_modes.shape
    margin, tiles = extent // 2, tile // LANES
    n_ty, n_tx = lax.axis_size("ty"), lax.axis_size("tx")
    rounds = pairings(n_ty)
    sizes = (n_ty, n_tx, rounds)
    parts = slices * 2 * tiles
    k_n = len(rounds)
    places = positions.T
    planes = slices * 2
    block = (margin, LANES)
    ext_shape = (planes, tiles + 2, tile + extent, LANES)
    strips = [pltpu.VMEM((slices, tile, LANES), BF16)] * 2
    strips = [pltpu.VMEM((slices, tile, LANES), BF16)] * 2
    rows_out = [pltpu.VMEM((parts + 2 * slices,) + block, BF16)] * 2
    ty_a, ty_b, tx_a, tx_b, near_patterns, ext, grad, *routed = call(
        lambda *r: pack_kernel(sizes, *r),
        (far(object_slices), far(patterns), far(places), far(counts)),
        [ANY] * 4,
        [pltpu.VMEM((parts + extra,) + block, BF16) for extra in (2 * CAP, 0)]
        + strips
        + [pltpu.VMEM(patterns.shape, BF16)]
        + [pltpu.VMEM(ext_shape, F32)] * 2
        + [pltpu.VMEM((CAP, extent, extent), BF16)] * (k_n - 1),
        [
            pltpu.VMEM((2, slices, 2, margin, tile), F32),
            pltpu.SMEM(places.shape, jnp.int32),
            pltpu.SMEM(counts.shape, jnp.int32),
            pltpu.SemaphoreType.DMA((5 + 2 * planes,)),
        ],
    )
    near_object, near_patterns = near(object_slices), near(near_patterns)

    def pair_rows(value, k):
        return send(value, "ty", [(i, rounds[k][i]) for i in range(n_ty)])

    def swap(value, axis, side):
        return send(value, axis, neighbour_pairs(side, lax.axis_size(axis)))

    def cross(value, k):
        return send(value, "tx", [(i, i ^ k) for i in range(n_tx)])

    ty_in = [swap(ty_a, "ty", 0), swap(ty_b, "ty", 1)]
    tx_in = [swap(tx_a, "tx", 0), swap(tx_b, "tx", 1)]
    tables = make_tables(extent)
    ext, first, second, kern = call(
        tile_kernel,
        (far(object_slices),) + tuple(far(c) for c in tables) + (near(ext),),
        [ANY] * 4 + [VMEM],
        [pltpu.VMEM(ext_shape, F32)] + [pltpu.VMEM(c.shape, c.dtype) for c in tables],
        [pltpu.SemaphoreType.DMA((parts + 3,))],
        {4: 0},
    )
    constants = tuple(near(c) for c in (first, second, kern))
    corners = call(
        lambda *r: corner_kernel(slices, tiles, *r),
        tuple(ty_in),
        [VMEM] * 2,
        [pltpu.VMEM((2 * slices,) + block, BF16)] * 2,
    )
    corner_in = [swap(corners[j], "tx", j) for j in range(2)]
    pat_in = [ty_in[0]] + [pair_rows(routed[k - 1], k) for k in range(1, k_n)]

    slots = (k_n + 1) * CAP
    chunk = modes * 2 * extent // n_tx
    field = (slots, 2 * modes, extent, extent)
    places_near = [pltpu.SMEM((slots,), jnp.int32)] * 2
    ext, psi, waves = call(
        lambda *r: forward_kernel(sizes, patterns.shape[0], *r),
        (places, counts, near(probe_modes))
        + constants
        + tuple(ty_in + tx_in + corner_in)
        + (near(ext),),
        [SMEM, SMEM] + [VMEM] * 11,
        [pltpu.VMEM(ext_shape, F32), pltpu.VMEM(field, F32), pltpu.VMEM((slices - 1,) + field, F32)],
        places_near,
        {12: 0},
    )
    results = call(
        lambda *r: backward_kernel(sizes, *r),
        (near_patterns, places, counts, near(probe_modes))
        + constants
        + (near(ext), near(psi), near(waves), *pat_in, near(grad)),
        [VMEM, SMEM, SMEM] + [VMEM] * (7 + k_n + 1),
        [pltpu.VMEM(ext_shape, F32)]
        + rows_out
        + [pltpu.VMEM((n_tx // 2, chunk, LANES), F32)] * 2,
        [pltpu.VMEM((slots, extent, extent), BF16), pltpu.VMEM((2 * modes, extent, extent), F32)]
        + places_near
        + [pltpu.SMEM((slots,), F32)],
        {10 + k_n: 0},
    )
    grad, ty_a, ty_b, keep, share = results
    ty_back = [swap(ty_a, "ty", 0), swap(ty_b, "ty", 1)]
    mine, *shares = call(
        pair_kernel,
        (near(keep), cross(share, 1)),
        [VMEM] * 2,
        [pltpu.VMEM((chunk, LANES), F32)] + [pltpu.VMEM((chunk, LANES), BF16)] * (n_tx // 2 - 1),
    )
    others = tuple(cross(shares[k - 1], 2 * k) for k in range(1, n_tx // 2))
    mine = call(
        share_kernel, (near(mine),) + others, [VMEM] * (n_tx // 2), pltpu.VMEM((chunk, LANES), BF16)
    )
    rows_in = tuple(pair_rows(mine, k) for k in range(k_n))
    tx_a, tx_b, grad = call(
        lambda *r: fold_kernel(tile, *r),
        (near(grad), *ty_back),
        [VMEM] * 3,
        strips + [pltpu.VMEM(ext_shape, F32)],
        (),
        {0: 2},
    )
    tx_back = [swap(tx_a, "tx", 0), swap(tx_b, "tx", 1)]
    full = call(
        lambda *r: sum_kernel(sizes, *r),
        (near(mine),) + rows_in,
        [VMEM] * (k_n + 1),
        pltpu.VMEM((chunk, LANES), BF16),
        [pltpu.VMEM((n_ty, chunk, LANES), F32)],
    )
    gathered = tuple(cross(full, 2 * k) for k in range(1, n_tx // 2))
    joined = call(
        join_kernel,
        (near(full),) + gathered,
        [VMEM] * (n_tx // 2),
        pltpu.VMEM((n_tx // 2, chunk, LANES), BF16),
    )
    other = cross(joined, 1)
    partial = call(
        middle_kernel,
        (near_object, near(grad), near(probe_modes)),
        [VMEM] * 3,
        pltpu.HBM(object_slices.shape, F32),
        [pltpu.VMEM((slices, 2, tile, tile - 2 * LANES), F32), pltpu.SemaphoreType.DMA((planes,))],
        None,
        ANY,
    )
    new_object = call(
        edges_kernel,
        (near_object, near(grad), *tx_back, near(probe_modes), far(partial)),
        [VMEM] * 5 + [ANY],
        pltpu.HBM(object_slices.shape, F32),
        [
            pltpu.VMEM((2, slices, 2, tile, LANES), F32),
            pltpu.SemaphoreType.DMA((2 * slices,)),
        ],
        {5: 0},
        ANY,
    )
    new_probe = call(
        probe_kernel,
        (near(probe_modes), near(joined), other),
        [VMEM] * 3,
        jax.ShapeDtypeStruct(probe_modes.shape, F32),
        [pltpu.VMEM((modes * 2 * extent, LANES), F32)],
    )
    return (new_object, new_probe)


def solution(mesh):
    return jax.shard_map(
        step,
        mesh=mesh,
        in_specs=(P(None, None, "ty", "tx"), P(), P(("ty", "tx"), None, None), P(), P()),
        out_specs=(P(None, None, "ty", "tx"), P()),
        check_vma=False,
    )
```
